512 devices in a mesh: node: 16 (over z, core), dp: 32 (over x, y).
Axes of the slice: x: 4, y: 8, z: 8, core: 2. Of those that a mesh axis runs over, the one named last changes fastest.
Arguments:
- out_grad: bfloat16 [65536, 2560], P(('node', 'dp')), may hold values from -3 to 3
- gate_prob: bfloat16 [65536, 6], P(('node', 'dp')), may hold values from 0.019897461 to 0.5
- presel_nodes: int32 [65536, 3], P(('node', 'dp')), may hold values from 0 to 15, as said below
- route_expert: int32 [65536, 6], P(('node', 'dp')), may hold values from 0 to 29, as said below
- route_slot: int32 [65536, 6], P(('node', 'dp')), may hold values from -1 to 79, as said below
- gate_pre: bfloat16 [40960, 768], P(('node', 'dp')), may hold values from -6 to 6
- up_pre: bfloat16 [40960, 768], P(('node', 'dp')), may hold values from -6 to 6
- down_weight: bfloat16 [16, 768, 2560], P('node'), may hold values from -0.21875 to 0.21875
Outputs:
- grad_gate: bfloat16 [40960, 768], P(('node', 'dp'))
- grad_up: bfloat16 [40960, 768], P(('node', 'dp'))
- grad_down: bfloat16 [16, 768, 2560], P('node', 'dp')
- grad_prob: float32 [65536, 6], P(('node', 'dp'))
The draws below stay inside these ranges and needn't reach their ends.
Inputs may be any that keep to these rules, and one draw needn't show every extreme that they name: `presel_nodes`: three different nodes for each token. `route_expert`: each token names 6 different numbers; number c stands for expert c % 10 of the node in column c // 10 of presel_nodes. `route_slot`: -1 wherever route_expert % 10 != 0. Call a route with route_expert % 10 == 0 and route_slot >= 0 active: active routes of the tokens of one data index to one node have distinct slots, and in every draw some such block uses all 80 slots; the tokens of one device have at most 16 active routes to one node, and in every draw some device has exactly 16.
All inputs are finite; a program needn't handle non-finite values.
Results may differ from the reference program's by a relative error of at most 0.015.
Values may be sent and summed in bfloat16 or wider, within the bound.
No kernel may reach another device: no remote copies, remote signals or barrier semaphores. Data moves between devices by JAX's collectives and lax.ppermute only.
A program may use at most 64 MiB of HBM per device.

```python
import math
import jax
import jax.numpy as jnp
from jax import lax

D = 2560
F = 768
EXP_NODE = 10
TOPK = 6
PRESEL = 3
TOK_DEV = 128
CAP = 80
SRC_CAP = 16
TOKENS = 65536
SLOTS = 40960
N_NODE = 16
N_DP = 32


def routing_tables(key):
    rows = TOK_DEV * N_NODE * N_DP
    node_numbering = jnp.arange(N_NODE, dtype=jnp.int32)
    heavy_experts = jax.random.randint(jax.random.fold_in(key, 101), (), 0, N_NODE)
    random_jitter = jax.random.randint(jax.random.fold_in(key, 102), (rows, N_NODE), 0, 1 << 16)
    favoured_experts = jax.random.randint(jax.random.fold_in(key, 103), (rows, 1), 0, 10) < 7
    preference_boost = jnp.where(favoured_experts & (node_numbering[None, :] == heavy_experts), 1 << 28, 0)
    routing_score = random_jitter * N_NODE + node_numbering[None, :] + preference_boost
    presel = jnp.argsort(-routing_score, axis=1)[:, :PRESEL].astype(jnp.int32)
    many = PRESEL * EXP_NODE
    cand_ids = jnp.arange(many, dtype=jnp.int32)
    cand_noise = jax.random.randint(jax.random.fold_in(key, 104), (rows, many), 0, 1 << 16)
    expert = jnp.argsort(-(cand_noise * many + cand_ids[None, :]), axis=1)[:, :TOPK].astype(jnp.int32)
    window = expert % EXP_NODE == 0
    target_node = jnp.take_along_axis(presel, expert // EXP_NODE, axis=1)
    onehot = ((target_node[:, :, None] == node_numbering[None, None, :]) & window[:, :, None]).astype(jnp.int32)
    per_source = onehot.reshape(N_NODE * N_DP, TOK_DEV * TOPK, N_NODE)
    source_rank = jnp.cumsum(per_source, axis=1) - 1
    kept = per_source * (source_rank < SRC_CAP).astype(jnp.int32)
    kept = kept.reshape(N_NODE, N_DP, TOK_DEV * TOPK, N_NODE)
    grouped = jnp.transpose(kept, (1, 0, 2, 3)).reshape(N_DP, N_NODE * TOK_DEV * TOPK, N_NODE)
    block_rank = jnp.cumsum(grouped, axis=1) - 1
    fitting = grouped * (block_rank < CAP).astype(jnp.int32)
    back_fit = jnp.transpose(fitting.reshape(N_DP, N_NODE, TOK_DEV * TOPK, N_NODE), (1, 0, 2, 3)).reshape(rows, TOPK, N_NODE)
    back_rank = jnp.transpose(block_rank.reshape(N_DP, N_NODE, TOK_DEV * TOPK, N_NODE), (1, 0, 2, 3)).reshape(rows, TOPK, N_NODE)
    active = jnp.sum(back_fit, axis=2) > 0
    rank_here = jnp.sum(back_rank * back_fit, axis=2)
    data_id = (jnp.arange(rows, dtype=jnp.int32) // TOK_DEV % N_DP)[:, None]
    block_index = target_node * N_DP + data_id
    perm_noise = jax.random.randint(jax.random.fold_in(key, 105), (N_NODE * N_DP, CAP), 0, 1 << 16)
    perms = jnp.argsort(perm_noise * CAP + jnp.arange(CAP, dtype=jnp.int32)[None, :], axis=1).astype(jnp.int32)
    flat_index = jnp.clip(block_index * CAP + rank_here, 0, N_NODE * N_DP * CAP - 1)
    slot = jnp.where(active, perms.reshape(-1)[flat_index], -1).astype(jnp.int32)
    return (presel, expert, slot)


def draw_presel_nodes(key, part):
    return routing_tables(key)[0]


def draw_route_expert(key, part):
    return routing_tables(key)[1]


def draw_route_slot(key, part):
    return routing_tables(key)[2]


def level_of(rng, dims, cuts, low, largest):
    level = 1.0
    for position, blocks in cuts:
        steps = jax.random.uniform(jax.random.fold_in(jax.random.fold_in(rng, 6), position), (blocks,), jnp.float32, low / len(cuts), largest / len(cuts))
        level = level * jnp.repeat(jnp.exp(steps), dims[position] // blocks).reshape((-1,) + (1,) * (len(dims) - 1 - position))
    return level


def scatter_about(key, shape, width, bound, pieces=(), held_as=jnp.bfloat16):
    level = level_of(key, shape, pieces, -0.22, 0.18) if pieces else 1.0
    array = jax.random.normal(key, shape, jnp.float32) * width * level
    return jnp.minimum(jnp.maximum(array, -bound), bound).astype(held_as)


def setup_inputs(seed: int = 0) -> dict:
    key_list = jax.random.split(jax.random.key(seed), 9)
    return {
        "out_grad": scatter_about(key_list[0], (TOKENS, D), 0.5, 3.0, ((0, 512),)),
        "gate_prob": jnp.clip(jnp.exp(math.log(0.5) - 3.224016 * jax.random.uniform(key_list[1], (TOKENS, TOPK), jnp.float32) ** level_of(key_list[1], (TOKENS, TOPK), ((0, 512),), -0.2, 0.2)), 0.019897461, 0.5).astype(jnp.bfloat16),
        "presel_nodes": draw_presel_nodes(jax.random.fold_in(key_list[8], 71), 0),
        "route_expert": draw_route_expert(jax.random.fold_in(key_list[8], 71), 0),
        "route_slot": draw_route_slot(jax.random.fold_in(key_list[8], 71), 0),
        "gate_pre": scatter_about(key_list[5], (SLOTS, F), 1.0, 6.0, ((0, 512),)),
        "up_pre": scatter_about(key_list[6], (SLOTS, F), 1.0, 6.0, ((0, 512),)),
        "down_weight": scatter_about(key_list[7], (N_NODE, F, D), F ** -0.5, 0.21875, ((0, 16),)),
    }


def reference(out_grad, gate_prob, presel_nodes, route_expert, route_slot, gate_pre, up_pre, down_weight):
    tokens = out_grad.shape[0]
    blocks = N_NODE * N_DP
    active = (route_expert % EXP_NODE == 0) & (route_slot >= 0)
    target_node = jnp.take_along_axis(presel_nodes, (route_expert // EXP_NODE).astype(jnp.int32), axis=1)
    data_id = ((jnp.arange(tokens, dtype=jnp.int32) // TOK_DEV) % N_DP)[:, None]
    slot_row = jnp.where(active, (target_node * N_DP + data_id) * CAP + route_slot, blocks * CAP).astype(jnp.int32)
    slot_dy = jnp.zeros((blocks * CAP, D), jnp.bfloat16)
    slot_p = jnp.zeros((blocks * CAP,), jnp.float32)
    for choice_k in range(TOPK):
        slot_dy = slot_dy.at[slot_row[:, choice_k]].set(out_grad, mode="drop")
        slot_p = slot_p.at[slot_row[:, choice_k]].set(gate_prob[:, choice_k].astype(jnp.float32), mode="drop")

    def one_node(node_id):
        weight = lax.dynamic_index_in_dim(down_weight, node_id, 0, keepdims=False)

        def one_block(summed, data_index):
            first = ((node_id * N_DP + data_index) * CAP).astype(jnp.int32)
            dy_rows = lax.dynamic_slice_in_dim(slot_dy, first, CAP, 0).astype(jnp.float32)
            slot_probs = lax.dynamic_slice_in_dim(slot_p, first, CAP, 0)
            gate_rows = lax.dynamic_slice_in_dim(gate_pre, first, CAP, 0).astype(jnp.float32)
            up_rows = lax.dynamic_slice_in_dim(up_pre, first, CAP, 0).astype(jnp.float32)
            sigmoid_gate = jax.nn.sigmoid(gate_rows)
            activated = gate_rows * sigmoid_gate
            hidden = (activated * up_rows).astype(jnp.bfloat16)
            scaled_scores = (slot_probs[:, None] * dy_rows).astype(jnp.bfloat16)
            d_hidden = lax.dot_general(scaled_scores, weight, (((1,), (1,)), ((), ())), preferred_element_type=jnp.float32)
            grad_gate_rows = (d_hidden * up_rows * sigmoid_gate * (1.0 + gate_rows * (1.0 - sigmoid_gate))).astype(jnp.bfloat16)
            grad_up_rows = (d_hidden * activated).astype(jnp.bfloat16)
            slot_out = jnp.dot(hidden, weight, preferred_element_type=jnp.float32)
            grad_p_rows = jnp.sum(dy_rows * slot_out, axis=1)
            partial_term = lax.dot_general(hidden, scaled_scores, (((0,), (0,)), ((), ())), preferred_element_type=jnp.float32)
            rounded = lax.optimization_barrier(partial_term.astype(jnp.bfloat16))
            return summed + rounded.astype(jnp.float32), (grad_gate_rows, grad_up_rows, grad_p_rows)

        summed, outputs = lax.scan(one_block, jnp.zeros((F, D), jnp.float32), jnp.arange(N_DP, dtype=jnp.int32))
        return summed.astype(jnp.bfloat16), outputs[0], outputs[1], outputs[2]

    grad_down, grad_gate, grad_up, slot_grad_p = lax.map(one_node, jnp.arange(N_NODE, dtype=jnp.int32))
    grad_gate = grad_gate.reshape(blocks * CAP, F)
    grad_up = grad_up.reshape(blocks * CAP, F)
    flat_grad_p = slot_grad_p.reshape(blocks * CAP)
    picked = flat_grad_p[jnp.clip(slot_row, 0, blocks * CAP - 1)]
    grad_prob = jnp.where(active, picked, jnp.float32(0.0))
    return grad_gate, grad_up, grad_down, grad_prob
```

```python
import jax
import jax.numpy as jnp
from jax import lax
from jax.experimental import pallas as pl
from jax.experimental.pallas import tpu as pltpu
from jax.sharding import Mesh
from jax.sharding import PartitionSpec as P

EXP_NODE = 10
PRESEL = 3
SRC_CAP = 16
LANES = 128
NODE_DP = ("node", "dp_0", "dp_1")
F32 = jnp.float32
BF16 = jnp.bfloat16


def columns_of_routes(expert, slot, value):
    rows = []
    for c in range(PRESEL):
        named = (expert == c * EXP_NODE) & (slot >= 0)
        rows.append(jnp.sum(jnp.where(named, value, 0), axis=0, keepdims=True))
    return rows


def route_kernel(og_ref, prob_ref, presel_ref, expert_ref, slot_ref, send_ref):
    tokens, features = og_ref.shape
    n_node = send_ref.shape[0] // SRC_CAP
    expert, slot, presel = expert_ref[...], slot_ref[...], presel_ref[...]
    slots = columns_of_routes(expert, slot, slot + 1)
    probs = columns_of_routes(expert, slot, prob_ref[...].astype(F32))
    node_ids = lax.broadcasted_iota(jnp.int32, (n_node, tokens), 0)
    slot_to = jnp.zeros((n_node, tokens), F32)
    prob_to = jnp.zeros((n_node, tokens), F32)
    for c in range(PRESEL):
        here = presel[c : c + 1] == node_ids
        slot_to += jnp.where(here, slots[c].astype(F32), 0.0)
        prob_to += jnp.where(here, probs[c], 0.0)
    sent = slot_to > 0.0
    before = lax.broadcasted_iota(jnp.int32, (tokens, tokens), 0) < lax.broadcasted_iota(
        jnp.int32, (tokens, tokens), 1
    )
    rank = jnp.dot(
        jnp.where(sent, 1.0, 0.0).astype(BF16),
        jnp.where(before, 1.0, 0.0).astype(BF16),
        preferred_element_type=F32,
    )
    rank = jnp.where(sent, rank, -1.0)
    place = lax.broadcasted_iota(jnp.int32, (n_node, SRC_CAP, tokens), 1).astype(F32)
    picked = rank[:, None, :] == place
    rows = n_node * SRC_CAP
    slot_rows = jnp.sum(jnp.where(picked, slot_to[:, None, :], 0.0), axis=2, keepdims=True)
    prob_rows = jnp.sum(jnp.where(picked, prob_to[:, None, :], 0.0), axis=2, keepdims=True)
    lane = lax.broadcasted_iota(jnp.int32, (n_node, SRC_CAP, LANES), 2)
    info = jnp.where(lane == 0, slot_rows, jnp.where(lane == 1, prob_rows, 0.0))
    send_ref[:, features:] = info.reshape(rows, LANES).astype(BF16)
    pick = jnp.where(picked, 1.0, 0.0).reshape(rows, tokens).astype(BF16)
    send_ref[:, :features] = jnp.dot(pick, og_ref[...], preferred_element_type=F32).astype(BF16)


def land_kernel(recv_ref, out_ref, scaled_ref, parts_ref, grad_p_ref):
    capacity, features = scaled_ref.shape
    n_parts, _, width = parts_ref.shape
    recv = recv_ref[...]
    slot = recv_ref[:, features : features + 1].astype(F32)
    lane = lax.broadcasted_iota(jnp.int32, (recv.shape[0], LANES), 1).astype(F32)
    landing = jnp.where(slot == lane + 1.0, 1.0, 0.0).astype(BF16)
    landed = lax.dot_general(
        landing, recv, (((0,), (0,)), ((), ())), preferred_element_type=F32
    )[:capacity]
    dy = landed[:, :features]
    p = landed[:, features + 1 : features + 2]
    scaled = (p * dy).astype(BF16)
    scaled_ref[...] = scaled
    for k in range(n_parts):
        parts_ref[k] = scaled[:, k * width : (k + 1) * width]
    grad_p = jnp.sum(dy * out_ref[...], axis=1, keepdims=True)
    row = lax.broadcasted_iota(jnp.int32, (capacity, LANES), 0)
    column = lax.broadcasted_iota(jnp.int32, (capacity, LANES), 1)
    grad_p_ref[...] = jnp.sum(jnp.where(row == column, grad_p, 0.0), axis=0, keepdims=True)


def partial_kernel(me_ref, scaled_ref, *refs):
    *hidden_refs, out_ref = refs
    n = len(hidden_refs)
    total = None
    for k, hidden_ref in enumerate(hidden_refs):
        block = lax.rem(me_ref[0] - k + n, n)
        term = lax.dot_general(
            hidden_ref[...],
            scaled_ref[block],
            (((0,), (0,)), ((), ())),
            preferred_element_type=F32,
        )
        total = term if total is None else total + term
    out_ref[...] = total.astype(BF16).reshape(out_ref.shape)


def sum_kernel(terms_ref, out_ref):
    n, _, width = terms_ref.shape
    n_parts = out_ref.shape[1] // width
    each = n // n_parts
    for k in range(n_parts):
        total = terms_ref[k * each].astype(F32)
        for j in range(1, each):
            total += terms_ref[k * each + j].astype(F32)
        out_ref[:, k * width : (k + 1) * width] = total.astype(BF16)


def return_kernel(me_ref, grad_p_ref, presel_ref, expert_ref, slot_ref, out_ref):
    n_node = grad_p_ref.shape[0]
    tokens = presel_ref.shape[1]
    expert, slot, presel = expert_ref[...], slot_ref[...], presel_ref[...]
    slots = columns_of_routes(expert, slot, slot + 1)
    node_ids = lax.broadcasted_iota(jnp.int32, (n_node, tokens), 0)
    slot_ids = lax.broadcasted_iota(jnp.int32, (LANES, tokens), 0)
    result = jnp.zeros(out_ref.shape, F32)
    for c in range(PRESEL):
        here = (presel[c : c + 1] ^ me_ref[0]) == node_ids
        by_slot = lax.dot_general(
            grad_p_ref[...],
            jnp.where(here, 1.0, 0.0),
            (((0,), (0,)), ((), ())),
            preferred_element_type=F32,
            precision=lax.Precision.HIGHEST,
        )
        value = jnp.sum(jnp.where(slot_ids + 1 == slots[c], by_slot, 0.0), axis=0, keepdims=True)
        result += jnp.where((expert == c * EXP_NODE) & (slot >= 0), value, 0.0)
    out_ref[...] = result


VMEM = pl.BlockSpec(memory_space=pltpu.VMEM)
SMEM = pl.BlockSpec(memory_space=pltpu.SMEM)


def call(kernel, out_shape, in_specs):
    many = isinstance(out_shape, (tuple, list))
    return pl.pallas_call(
        kernel,
        out_shape=out_shape,
        in_specs=in_specs,
        out_specs=[VMEM] * len(out_shape) if many else VMEM,
        compiler_params=pltpu.CompilerParams(vmem_limit_bytes=12 * 1024 * 1024),
    )


def exchange(value, axes):
    return lax.all_to_all(value, axes, split_axis=0, concat_axis=0, tiled=True)


def step_of(
    out_grad, gate_prob, presel_nodes, route_expert, route_slot, gate_pre, up_pre, down_weight
):
    _, features = out_grad.shape
    capacity, units = gate_pre.shape
    n_node, n_0, n_1 = (lax.axis_size(a) for a in NODE_DP)
    width = features // n_0
    share = units // (n_0 * n_1)
    shape = jax.ShapeDtypeStruct
    presel, expert, slot = presel_nodes.T, route_expert.T, route_slot.T

    send = call(
        route_kernel, shape((n_node * SRC_CAP, features + LANES), BF16), [VMEM] * 5
    )(out_grad, gate_prob.T, presel, expert, slot)
    recv = exchange(send.reshape(n_node, SRC_CAP, features + LANES), "node")
    recv = recv.reshape(n_node * SRC_CAP, features + LANES)

    weight = down_weight[0]
    gate_rows = gate_pre.astype(F32)
    up_rows = up_pre.astype(F32)
    sigmoid_gate = jax.nn.sigmoid(gate_rows)
    activated = gate_rows * sigmoid_gate
    hidden = (activated * up_rows).astype(BF16)
    hiddens = [hidden]
    for k in range(1, n_0):
        hiddens.append(
            lax.ppermute(hidden, "dp_0", [(i, (i + k) % n_0) for i in range(n_0)])
        )
    slot_out = jnp.dot(hidden, weight, preferred_element_type=F32)

    scaled, parts, grad_p = call(
        land_kernel,
        [
            shape((capacity, features), BF16),
            shape((n_0, capacity, width), BF16),
            shape((1, LANES), F32),
        ],
        [VMEM] * 2,
    )(recv, slot_out)
    parts = exchange(parts, "dp_0")

    d_hidden = lax.dot_general(
        scaled, weight, (((1,), (1,)), ((), ())), preferred_element_type=F32
    )
    grad_gate = (
        d_hidden * up_rows * sigmoid_gate * (1.0 + gate_rows * (1.0 - sigmoid_gate))
    ).astype(BF16)
    grad_up = (d_hidden * activated).astype(BF16)

    partial = call(
        partial_kernel, shape((n_0 * n_1, share, width), BF16), [SMEM] + [VMEM] * (1 + n_0)
    )(lax.axis_index("dp_0")[None], parts, *hiddens)
    terms = exchange(partial, ("dp_0", "dp_1"))
    grad_down = call(sum_kernel, shape((share, features), BF16), [VMEM])(terms)[None]

    step = 1
    while step < n_node:
        other = lax.ppermute(grad_p, "node", [(i, i ^ step) for i in range(n_node)])
        grad_p = jnp.concatenate([grad_p, other])
        step *= 2
    grad_prob = call(
        return_kernel, shape(route_expert.shape[::-1], F32), [SMEM] + [VMEM] * 4
    )(lax.axis_index("node")[None], grad_p, presel, expert, slot).T
    return (grad_gate, grad_up, grad_down, grad_prob)


def solution(mesh):
    finer = Mesh(mesh.devices.reshape(mesh.shape["node"], 4, 8), NODE_DP)
    in_specs = (P(NODE_DP, None),) * 7 + (P("node", None, None),)
    out_specs = (
        P(NODE_DP, None),
        P(NODE_DP, None),
        P("node", ("dp_0", "dp_1"), None),
        P(NODE_DP, None),
    )
    return jax.shard_map(
        step_of, mesh=finer, in_specs=in_specs, out_specs=out_specs, check_vma=False
    )
```

```python
import functools

import jax
import jax.numpy as jnp
from jax import lax
from jax.experimental import pallas as pl
from jax.experimental.pallas import tpu as pltpu
from jax.sharding import Mesh
from jax.sharding import PartitionSpec as P

EXP_NODE = 10
PRESEL = 3
SRC_CAP = 16
LANES = 128
DP = ("dp_0", "dp_1", "dp_2")
NODE_DP = ("node", *DP)
TEAM = ("dp_0", "dp_2")
HALF = LANES // 2
F32 = jnp.float32
BF16 = jnp.bfloat16


def columns_of_routes(expert, slot, value):
    rows = []
    for c in range(PRESEL):
        named = (expert == c * EXP_NODE) & (slot >= 0)
        rows.append(jnp.sum(jnp.where(named, value, 0), axis=0, keepdims=True))
    return rows


def route_kernel(*refs):
    sources, send_ref, held, arrived = refs[:5], refs[5], refs[6:11], refs[11]
    copies = [
        pltpu.make_async_copy(source, place, arrived.at[i])
        for i, (source, place) in enumerate(zip(sources, held))
    ]
    for copy in reversed(copies):
        copy.start()
    for copy in reversed(copies[1:]):
        copy.wait()
    og_ref, prob_ref, presel_ref, expert_ref, slot_ref = held
    tokens, features = og_ref.shape
    n_node = send_ref.shape[0] // SRC_CAP
    expert, slot, presel = expert_ref[...], slot_ref[...], presel_ref[...]
    slots = columns_of_routes(expert, slot, slot + 1)
    probs = columns_of_routes(expert, slot, prob_ref[...].astype(F32))
    node_ids = lax.broadcasted_iota(jnp.int32, (n_node, tokens), 0)
    slot_to = jnp.zeros((n_node, tokens), F32)
    prob_to = jnp.zeros((n_node, tokens), F32)
    for c in range(PRESEL):
        here = presel[c : c + 1] == node_ids
        slot_to += jnp.where(here, slots[c].astype(F32), 0.0)
        prob_to += jnp.where(here, probs[c], 0.0)
    sent = slot_to > 0.0
    before = lax.broadcasted_iota(jnp.int32, (tokens, tokens), 0) < lax.broadcasted_iota(
        jnp.int32, (tokens, tokens), 1
    )
    rank = jnp.dot(
        jnp.where(sent, 1.0, 0.0).astype(BF16),
        jnp.where(before, 1.0, 0.0).astype(BF16),
        preferred_element_type=F32,
    )
    rank = jnp.where(sent, rank, -1.0)
    place = lax.broadcasted_iota(jnp.int32, (n_node, SRC_CAP, tokens), 1).astype(F32)
    picked = rank[:, None, :] == place
    rows = n_node * SRC_CAP
    slot_rows = jnp.sum(jnp.where(picked, slot_to[:, None, :], 0.0), axis=2, keepdims=True)
    prob_rows = jnp.sum(jnp.where(picked, prob_to[:, None, :], 0.0), axis=2, keepdims=True)
    lane = lax.broadcasted_iota(jnp.int32, (n_node, SRC_CAP, LANES), 2)
    info = jnp.where(lane == 0, slot_rows, jnp.where(lane == 1, prob_rows, 0.0))
    send_ref[:, features:] = info.reshape(rows, LANES).astype(BF16)
    pick = jnp.where(picked, 1.0, 0.0).reshape(rows, tokens).astype(BF16)
    copies[0].wait()
    send_ref[:, :features] = jnp.dot(pick, og_ref[...], preferred_element_type=F32).astype(BF16)


def land_kernel(recv_ref, out_ref, scaled_ref, parts_ref, grad_p_ref):
    capacity, features = scaled_ref.shape
    recv = recv_ref[...]
    slot = recv_ref[:, features : features + 1].astype(F32)
    lane = lax.broadcasted_iota(jnp.int32, (recv.shape[0], LANES), 1).astype(F32)
    landing = jnp.where(slot == lane + 1.0, 1.0, 0.0).astype(BF16)
    landed = lax.dot_general(
        landing, recv, (((0,), (0,)), ((), ())), preferred_element_type=F32
    )[:capacity]
    dy = landed[:, :features]
    p = landed[:, features + 1 : features + 2]
    scaled = (p * dy).astype(BF16)
    scaled_ref[...] = scaled
    n = parts_ref.shape[0]
    rows = capacity // 2
    low = lax.broadcasted_iota(jnp.int32, (rows, LANES), 1) < HALF
    for k in range(n):
        for j in range(2):
            tile = 2 * k + j
            parts_ref[k, j * capacity : (j + 1) * capacity] = scaled[
                :, tile * LANES : (tile + 1) * LANES
            ]
    for k in range(n):
        tile = 2 * n + k // 2
        own = (p * dy[:, tile * LANES : (tile + 1) * LANES])
        swapped = pltpu.roll(own, HALF, 1)
        top, bottom = (own, swapped) if k % 2 == 0 else (swapped, own)
        parts_ref[k, 2 * capacity :] = jnp.where(low, top[:rows], bottom[rows:]).astype(BF16)
    grad_p = jnp.sum(dy * out_ref[...], axis=1, keepdims=True)
    row = lax.broadcasted_iota(jnp.int32, (capacity, LANES), 0)
    column = lax.broadcasted_iota(jnp.int32, (capacity, LANES), 1)
    grad_p_ref[...] = jnp.sum(jnp.where(row == column, grad_p, 0.0), axis=0, keepdims=True)


def partial_kernel(me_ref, parts_ref, *refs):
    *hidden_refs, out_ref = refs
    n_0 = len(hidden_refs)
    capacity = hidden_refs[0].shape[1]
    total = None
    for k, hidden_ref in enumerate(hidden_refs):
        for j in range(2):
            block = lax.rem(me_ref[0] - k + n_0, n_0) * 2 + (me_ref[1] ^ j)
            packed = parts_ref[block, 2 * capacity :].astype(F32)
            halves = jnp.concatenate([packed, pltpu.roll(packed, HALF, 1)]).astype(BF16)
            scaled = jnp.concatenate(
                [parts_ref[block, :capacity], parts_ref[block, capacity : 2 * capacity], halves],
                axis=1,
            )
            term = lax.dot_general(
                hidden_ref[j], scaled, (((0,), (0,)), ((), ())), preferred_element_type=F32
            )
            total = term if total is None else total + term
    n = out_ref.shape[0]
    share = total.shape[0] // n
    total = total.reshape(n, share, 3 * LANES)
    out_ref[:, :share] = total[:, :, :LANES].astype(BF16)
    out_ref[:, share : 2 * share] = total[:, :, LANES : 2 * LANES].astype(BF16)
    third = share // 3
    last = total[:, :, 2 * LANES :]
    low = lax.broadcasted_iota(jnp.int32, (n, third, LANES), 2) < HALF
    swapped = pltpu.roll(last[:, third : 2 * third], HALF, 2)
    mixed = jnp.where(low, last[:, :third], swapped)
    out_ref[:, 2 * share : 2 * share + third] = mixed.astype(BF16)
    out_ref[:, 2 * share + third :] = last[:, 2 * third :].astype(BF16)


def sum_kernel(n_0, n_1, terms_ref, out_ref):
    share = out_ref.shape[0]
    third = share // 3
    n = 2 * n_0
    low = lax.broadcasted_iota(jnp.int32, (third, LANES), 1) < HALF

    def put(row, tile, value):
        out_ref[row : row + value.shape[0], tile * LANES : (tile + 1) * LANES] = value.astype(BF16)

    for k in range(n_0):
        ends = []
        for j in range(2):
            total = None
            for i in range(n_1):
                term = terms_ref[(k * n_1 + i) * 2 + j].astype(F32)
                total = term if total is None else total + term
            tile = 2 * (2 * k + j)
            put(0, tile, total[:share])
            put(0, tile + 1, total[share : 2 * share])
            ends.append((total[2 * share : 2 * share + third], total[2 * share + third :]))
        (mixed_0, last_0), (mixed_1, last_1) = ends
        tile = 2 * n + k
        put(0, tile, jnp.where(low, mixed_0, pltpu.roll(mixed_1, HALF, 1)))
        put(third, tile, jnp.where(low, pltpu.roll(mixed_0, HALF, 1), mixed_1))
        put(2 * third, tile, jnp.where(low, last_0, pltpu.roll(last_1, HALF, 1)))


def return_kernel(me_ref, grad_p_ref, presel_ref, expert_ref, slot_ref, out_ref):
    n_node = grad_p_ref.shape[0]
    tokens = presel_ref.shape[1]
    expert, slot, presel = expert_ref[...], slot_ref[...], presel_ref[...]
    slots = columns_of_routes(expert, slot, slot + 1)
    node_ids = lax.broadcasted_iota(jnp.int32, (n_node, tokens), 0)
    slot_ids = lax.broadcasted_iota(jnp.int32, (LANES, tokens), 0)
    result = jnp.zeros(out_ref.shape, F32)
    for c in range(PRESEL):
        here = (presel[c : c + 1] ^ me_ref[0]) == node_ids
        by_slot = lax.dot_general(
            grad_p_ref[...],
            jnp.where(here, 1.0, 0.0),
            (((0,), (0,)), ((), ())),
            preferred_element_type=F32,
            precision=lax.Precision.HIGHEST,
        )
        value = jnp.sum(jnp.where(slot_ids + 1 == slots[c], by_slot, 0.0), axis=0, keepdims=True)
        result += jnp.where((expert == c * EXP_NODE) & (slot >= 0), value, 0.0)
    out_ref[...] = result


HBM = pl.BlockSpec(memory_space=pltpu.HBM)
VMEM = pl.BlockSpec(memory_space=pltpu.VMEM)
SMEM = pl.BlockSpec(memory_space=pltpu.SMEM)


def call(kernel, out_shape, in_specs, scratch=(), vmem_mib=12):
    many = isinstance(out_shape, (tuple, list))
    return pl.pallas_call(
        kernel,
        out_shape=out_shape,
        in_specs=in_specs,
        out_specs=[VMEM] * len(out_shape) if many else VMEM,
        scratch_shapes=scratch,
        compiler_params=pltpu.CompilerParams(vmem_limit_bytes=vmem_mib << 20),
    )


def exchange(value, axes):
    return lax.all_to_all(value, axes, split_axis=0, concat_axis=0, tiled=True)


def step_of(
    out_grad, gate_prob, presel_nodes, route_expert, route_slot, gate_pre, up_pre, down_weight
):
    _, features = out_grad.shape
    capacity, units = gate_pre.shape
    n_node, n_0, n_1, n_2 = (lax.axis_size(a) for a in NODE_DP)
    team = n_0 * n_2
    group = team * n_1
    share = units // group
    shape = jax.ShapeDtypeStruct
    presel, expert, slot = presel_nodes.T, route_expert.T, route_slot.T
    routed = (out_grad, gate_prob.T, presel, expert, slot)

    send = call(
        route_kernel,
        shape((n_node * SRC_CAP, features + LANES), BF16),
        [HBM] * 5,
        [pltpu.VMEM(a.shape, a.dtype) for a in routed] + [pltpu.SemaphoreType.DMA((5,))],
        vmem_mib=60,
    )(*routed)
    recv = exchange(send.reshape(n_node, SRC_CAP, features + LANES), "node")
    recv = recv.reshape(n_node * SRC_CAP, features + LANES)

    weight = down_weight[0]
    gate_rows = gate_pre.astype(F32)
    up_rows = up_pre.astype(F32)
    sigmoid_gate = jax.nn.sigmoid(gate_rows)
    activated = gate_rows * sigmoid_gate
    hidden = (activated * up_rows).astype(BF16)
    near = lax.ppermute(hidden, "dp_2", [(0, 1), (1, 0)])
    hidden_pair = jnp.stack([hidden, near])
    hiddens = [hidden_pair]
    for k in range(1, n_0):
        hiddens.append(lax.ppermute(hidden_pair, "dp_0", [(i, (i + k) % n_0) for i in range(n_0)]))
    slot_out = jnp.dot(hidden, weight, preferred_element_type=F32)

    scaled, parts, grad_p = call(
        land_kernel,
        [
            shape((capacity, features), BF16),
            shape((team, features * capacity // (team * LANES), LANES), BF16),
            shape((1, LANES), F32),
        ],
        [VMEM] * 2,
    )(recv, slot_out)
    parts = exchange(parts, TEAM)

    d_hidden = lax.dot_general(scaled, weight, (((1,), (1,)), ((), ())), preferred_element_type=F32)
    grad_gate = (
        d_hidden * up_rows * sigmoid_gate * (1.0 + gate_rows * (1.0 - sigmoid_gate))
    ).astype(BF16)
    grad_up = (d_hidden * activated).astype(BF16)

    partial = call(
        partial_kernel,
        shape((group, 2 * share + 2 * share // 3, LANES), BF16),
        [SMEM] + [VMEM] * (1 + n_0),
    )(jnp.stack([lax.axis_index(a) for a in TEAM]), parts, *hiddens)
    terms = exchange(partial, DP)
    grad_down = call(
        functools.partial(sum_kernel, n_0, n_1), shape((share, features), BF16), [VMEM]
    )(terms)[None]

    step = 1
    while step < n_node:
        other = lax.ppermute(grad_p, "node", [(i, i ^ step) for i in range(n_node)])
        grad_p = jnp.concatenate([grad_p, other])
        step *= 2
    grad_prob = call(
        return_kernel, shape(route_expert.shape[::-1], F32), [SMEM] + [VMEM] * 4
    )(lax.axis_index("node")[None], grad_p, presel, expert, slot).T
    return (grad_gate, grad_up, grad_down, grad_prob)


def solution(mesh):
    finer = Mesh(mesh.devices.reshape(mesh.shape["node"], 4, 4, 2), NODE_DP)
    in_specs = (P(NODE_DP, None),) * 7 + (P("node", None, None),)
    out_specs = (
        P(NODE_DP, None),
        P(NODE_DP, None),
        P("node", DP, None),
        P(NODE_DP, None),
    )
    return jax.shard_map(
        step_of, mesh=finer, in_specs=in_specs, out_specs=out_specs, check_vma=False
    )
```

```python
import functools

import jax
import jax.numpy as jnp
from jax import lax
from jax.experimental import pallas as pl
from jax.experimental.pallas import tpu as pltpu
from jax.sharding import Mesh
from jax.sharding import PartitionSpec as P

EXP_NODE = 10
PRESEL = 3
SRC_CAP = 16
LANES = 128
DP = ("dp_0", "dp_1", "dp_2")
NODE_DP = ("node", *DP)
TEAM = ("dp_0", "dp_2")
HALF = LANES // 2
F32 = jnp.float32
BF16 = jnp.bfloat16


def columns_of_routes(expert, slot, value):
    rows = []
    for c in range(PRESEL):
        named = (expert == c * EXP_NODE) & (slot >= 0)
        rows.append(jnp.sum(jnp.where(named, value, 0), axis=0, keepdims=True))
    return rows


def route_kernel(*refs):
    sources, send_ref, held, arrived = refs[:5], refs[5], refs[6:11], refs[11]
    copies = [
        pltpu.make_async_copy(source, place, arrived.at[i])
        for i, (source, place) in enumerate(zip(sources, held))
    ]
    for copy in reversed(copies):
        copy.start()
    for copy in reversed(copies[1:]):
        copy.wait()
    og_ref, prob_ref, presel_ref, expert_ref, slot_ref = held
    tokens, features = og_ref.shape
    n_node = send_ref.shape[0] // SRC_CAP
    expert, slot, presel = expert_ref[...], slot_ref[...], presel_ref[...]
    slots = columns_of_routes(expert, slot, slot + 1)
    probs = columns_of_routes(expert, slot, prob_ref[...].astype(F32))
    node_ids = lax.broadcasted_iota(jnp.int32, (n_node, tokens), 0)
    slot_to = jnp.zeros((n_node, tokens), F32)
    prob_to = jnp.zeros((n_node, tokens), F32)
    for c in range(PRESEL):
        here = presel[c : c + 1] == node_ids
        slot_to += jnp.where(here, slots[c].astype(F32), 0.0)
        prob_to += jnp.where(here, probs[c], 0.0)
    sent = slot_to > 0.0
    before = lax.broadcasted_iota(jnp.int32, (tokens, tokens), 0) < lax.broadcasted_iota(
        jnp.int32, (tokens, tokens), 1
    )
    rank = jnp.dot(
        jnp.where(sent, 1.0, 0.0).astype(BF16),
        jnp.where(before, 1.0, 0.0).astype(BF16),
        preferred_element_type=F32,
    )
    rank = jnp.where(sent, rank, -1.0)
    place = lax.broadcasted_iota(jnp.int32, (n_node, SRC_CAP, tokens), 1).astype(F32)
    picked = rank[:, None, :] == place
    rows = n_node * SRC_CAP
    slot_rows = jnp.sum(jnp.where(picked, slot_to[:, None, :], 0.0), axis=2, keepdims=True)
    prob_rows = jnp.sum(jnp.where(picked, prob_to[:, None, :], 0.0), axis=2, keepdims=True)
    lane = lax.broadcasted_iota(jnp.int32, (n_node, SRC_CAP, LANES), 2)
    info = jnp.where(lane == 0, slot_rows, jnp.where(lane == 1, prob_rows, 0.0))
    send_ref[:, features:] = info.reshape(rows, LANES).astype(BF16)
    pick = jnp.where(picked, 1.0, 0.0).reshape(rows, tokens).astype(BF16)
    copies[0].wait()
    send_ref[:, :features] = jnp.dot(pick, og_ref[...], preferred_element_type=F32).astype(BF16)


def land_kernel(recv_ref, out_ref, scaled_ref, parts_ref, grad_p_ref):
    capacity, features = scaled_ref.shape
    recv = recv_ref[...]
    slot = recv_ref[:, features : features + 1].astype(F32)
    lane = lax.broadcasted_iota(jnp.int32, (recv.shape[0], LANES), 1).astype(F32)
    landing = jnp.where(slot == lane + 1.0, 1.0, 0.0).astype(BF16)
    landed = lax.dot_general(
        landing, recv, (((0,), (0,)), ((), ())), preferred_element_type=F32
    )[:capacity]
    dy = landed[:, :features]
    p = landed[:, features + 1 : features + 2]
    scaled = (p * dy).astype(BF16)
    scaled_ref[...] = scaled
    n = parts_ref.shape[0]
    rows = capacity // 2
    low = lax.broadcasted_iota(jnp.int32, (rows, LANES), 1) < HALF
    for k in range(n):
        for j in range(2):
            tile = 2 * k + j
            parts_ref[k, j * capacity : (j + 1) * capacity] = scaled[
                :, tile * LANES : (tile + 1) * LANES
            ]
    for k in range(n):
        tile = 2 * n + k // 2
        own = (p * dy[:, tile * LANES : (tile + 1) * LANES])
        swapped = pltpu.roll(own, HALF, 1)
        top, bottom = (own, swapped) if k % 2 == 0 else (swapped, own)
        parts_ref[k, 2 * capacity :] = jnp.where(low, top[:rows], bottom[rows:]).astype(BF16)
    grad_p = jnp.sum(dy * out_ref[...], axis=1, keepdims=True)
    row = lax.broadcasted_iota(jnp.int32, (capacity, LANES), 0)
    column = lax.broadcasted_iota(jnp.int32, (capacity, LANES), 1)
    grad_p_ref[...] = jnp.sum(jnp.where(row == column, grad_p, 0.0), axis=0, keepdims=True)


def collect_kernel(me_ref, *refs):
    *hidden_refs, out_ref, rows_ref = refs
    n_0 = len(hidden_refs)
    capacity = hidden_refs[0].shape[1]
    for k, hidden_ref in enumerate(hidden_refs):
        for j in range(2):
            block = lax.rem(me_ref[0] - k + n_0, n_0) * 2 + (me_ref[1] ^ j)
            start = pl.multiple_of(block * capacity, capacity)
            rows_ref[pl.ds(start, capacity)] = hidden_ref[j].astype(F32)
    out_ref[...] = rows_ref[...].T.astype(BF16)


def partial_kernel(hidden_ref, parts_ref, out_ref):
    team, rows, _ = parts_ref.shape
    capacity = rows * 2 // 5
    blocks = []
    for block in range(team):
        packed = parts_ref[block, 2 * capacity :].astype(F32)
        halves = jnp.concatenate([packed, pltpu.roll(packed, HALF, 1)]).astype(BF16)
        blocks.append(
            jnp.concatenate(
                [parts_ref[block, :capacity], parts_ref[block, capacity : 2 * capacity], halves],
                axis=1,
            )
        )
    total = jnp.dot(hidden_ref[...], jnp.concatenate(blocks), preferred_element_type=F32)
    n = out_ref.shape[0]
    share = total.shape[0] // n
    total = total.reshape(n, share, 3 * LANES)
    out_ref[:, :share] = total[:, :, :LANES].astype(BF16)
    out_ref[:, share : 2 * share] = total[:, :, LANES : 2 * LANES].astype(BF16)
    third = share // 3
    last = total[:, :, 2 * LANES :]
    low = lax.broadcasted_iota(jnp.int32, (n, third, LANES), 2) < HALF
    swapped = pltpu.roll(last[:, third : 2 * third], HALF, 2)
    mixed = jnp.where(low, last[:, :third], swapped)
    out_ref[:, 2 * share : 2 * share + third] = mixed.astype(BF16)
    out_ref[:, 2 * share + third :] = last[:, 2 * third :].astype(BF16)


def sum_kernel(n_0, n_1, terms_ref, out_ref):
    share = out_ref.shape[0]
    third = share // 3
    n = 2 * n_0
    low = lax.broadcasted_iota(jnp.int32, (third, LANES), 1) < HALF

    def put(row, tile, value):
        out_ref[row : row + value.shape[0], tile * LANES : (tile + 1) * LANES] = value.astype(BF16)

    for k in range(n_0):
        ends = []
        for j in range(2):
            total = None
            for i in range(n_1):
                term = terms_ref[(k * n_1 + i) * 2 + j].astype(F32)
                total = term if total is None else total + term
            tile = 2 * (2 * k + j)
            put(0, tile, total[:share])
            put(0, tile + 1, total[share : 2 * share])
            ends.append((total[2 * share : 2 * share + third], total[2 * share + third :]))
        (mixed_0, last_0), (mixed_1, last_1) = ends
        tile = 2 * n + k
        put(0, tile, jnp.where(low, mixed_0, pltpu.roll(mixed_1, HALF, 1)))
        put(third, tile, jnp.where(low, pltpu.roll(mixed_0, HALF, 1), mixed_1))
        put(2 * third, tile, jnp.where(low, last_0, pltpu.roll(last_1, HALF, 1)))


def grads_kernel(scaled_ref, gate_ref, up_ref, weight_ref, grad_gate_ref, grad_up_ref):
    d_hidden = lax.dot_general(
        scaled_ref[...], weight_ref[...], (((1,), (1,)), ((), ())), preferred_element_type=F32
    )
    gate, up = gate_ref[...].astype(F32), up_ref[...].astype(F32)
    sigmoid = jax.nn.sigmoid(gate)
    slope = sigmoid * (1.0 + gate * (1.0 - sigmoid))
    grad_gate_ref[...] = (d_hidden * up * slope).astype(BF16)
    grad_up_ref[...] = (d_hidden * (gate * sigmoid)).astype(BF16)


def return_kernel(steps, me_ref, grad_p_ref, presel_ref, expert_ref, slot_ref, out_ref):
    n_node = grad_p_ref.shape[0]
    tokens = presel_ref.shape[1]
    expert, slot, presel = expert_ref[...], slot_ref[...], presel_ref[...]
    slots = columns_of_routes(expert, slot, slot + 1)
    row = lax.broadcasted_iota(jnp.int32, (n_node, tokens), 0)
    away = jnp.zeros((n_node, tokens), jnp.int32)
    for bit, step in enumerate(steps):
        away = jnp.where((row >> bit) & 1 == 1, away | step, away)
    slot_ids = lax.broadcasted_iota(jnp.int32, (LANES, tokens), 0)
    result = jnp.zeros(out_ref.shape, F32)
    for c in range(PRESEL):
        here = (presel[c : c + 1] ^ me_ref[0]) == away
        by_slot = lax.dot_general(
            grad_p_ref[...],
            jnp.where(here, 1.0, 0.0),
            (((0,), (0,)), ((), ())),
            preferred_element_type=F32,
            precision=lax.Precision.HIGHEST,
        )
        value = jnp.sum(jnp.where(slot_ids + 1 == slots[c], by_slot, 0.0), axis=0, keepdims=True)
        result += jnp.where((expert == c * EXP_NODE) & (slot >= 0), value, 0.0)
    out_ref[...] = result


HBM = pl.BlockSpec(memory_space=pltpu.HBM)
VMEM = pl.BlockSpec(memory_space=pltpu.VMEM)
SMEM = pl.BlockSpec(memory_space=pltpu.SMEM)


def call(kernel, out_shape, in_specs, scratch=(), vmem_mib=12):
    many = isinstance(out_shape, (tuple, list))
    return pl.pallas_call(
        kernel,
        out_shape=out_shape,
        in_specs=in_specs,
        out_specs=[VMEM] * len(out_shape) if many else VMEM,
        scratch_shapes=scratch,
        compiler_params=pltpu.CompilerParams(vmem_limit_bytes=vmem_mib << 20),
    )


def exchange(value, axes):
    return lax.all_to_all(value, axes, split_axis=0, concat_axis=0, tiled=True)


def step_of(
    out_grad, gate_prob, presel_nodes, route_expert, route_slot, gate_pre, up_pre, down_weight
):
    _, features = out_grad.shape
    capacity, units = gate_pre.shape
    n_node, n_0, n_1, n_2 = (lax.axis_size(a) for a in NODE_DP)
    team = n_0 * n_2
    group = team * n_1
    share = units // group
    shape = jax.ShapeDtypeStruct
    presel, expert, slot = presel_nodes.T, route_expert.T, route_slot.T
    routed = (out_grad, gate_prob.T, presel, expert, slot)

    send = call(
        route_kernel,
        shape((n_node * SRC_CAP, features + LANES), BF16),
        [HBM] * 5,
        [pltpu.VMEM(a.shape, a.dtype) for a in routed] + [pltpu.SemaphoreType.DMA((5,))],
        vmem_mib=60,
    )(*routed)
    recv = exchange(send.reshape(n_node, SRC_CAP, features + LANES), "node")
    recv = recv.reshape(n_node * SRC_CAP, features + LANES)

    weight = down_weight[0]
    gate_rows = gate_pre.astype(F32)
    up_rows = up_pre.astype(F32)
    sigmoid_gate = jax.nn.sigmoid(gate_rows)
    activated = gate_rows * sigmoid_gate
    hidden = (activated * up_rows).astype(BF16)
    near = lax.ppermute(hidden, "dp_2", [(0, 1), (1, 0)])
    hidden_pair = jnp.stack([hidden, near])
    hiddens = [hidden_pair]
    for k in range(1, n_0):
        hiddens.append(lax.ppermute(hidden_pair, "dp_0", [(i, (i + k) % n_0) for i in range(n_0)]))
    team_hidden = call(
        collect_kernel,
        shape((units, team * capacity), BF16),
        [SMEM] + [VMEM] * n_0,
        [pltpu.VMEM((team * capacity, units), F32)],
    )(jnp.stack([lax.axis_index(a) for a in TEAM]), *hiddens)
    slot_out = jnp.dot(hidden, weight, preferred_element_type=F32)

    scaled, parts, grad_p = call(
        land_kernel,
        [
            shape((capacity, features), BF16),
            shape((team, features * capacity // (team * LANES), LANES), BF16),
            shape((1, LANES), F32),
        ],
        [VMEM] * 2,
    )(recv, slot_out)
    parts = exchange(parts, TEAM)

    grad_gate, grad_up = call(
        grads_kernel, [shape((capacity, units), BF16)] * 2, [VMEM] * 4
    )(scaled, gate_pre, up_pre, weight)

    partial = call(
        partial_kernel, shape((group, 2 * share + 2 * share // 3, LANES), BF16), [VMEM] * 2
    )(team_hidden, parts)
    terms = exchange(partial, DP)
    grad_down = call(
        functools.partial(sum_kernel, n_0, n_1), shape((share, features), BF16), [VMEM]
    )(terms)[None]

    steps = [n_node >> (i + 1) for i in range(n_node.bit_length() - 1)]
    for step in steps:
        other = lax.ppermute(grad_p, "node", [(i, i ^ step) for i in range(n_node)])
        grad_p = jnp.concatenate([grad_p, other])
    grad_prob = call(
        functools.partial(return_kernel, steps),
        shape(route_expert.shape[::-1], F32),
        [SMEM] + [VMEM] * 4,
    )(lax.axis_index("node")[None], grad_p, presel, expert, slot).T
    return (grad_gate, grad_up, grad_down, grad_prob)


def solution(mesh):
    finer = Mesh(mesh.devices.reshape(mesh.shape["node"], 4, 4, 2), NODE_DP)
    in_specs = (P(NODE_DP, None),) * 7 + (P("node", None, None),)
    out_specs = (
        P(NODE_DP, None),
        P(NODE_DP, None),
        P("node", DP, None),
        P(NODE_DP, None),
    )
    return jax.shard_map(
        step_of, mesh=finer, in_specs=in_specs, out_specs=out_specs, check_vma=False
    )
```

```python
import functools

import jax
import jax.numpy as jnp
from jax import lax
from jax.experimental import pallas as pl
from jax.experimental.pallas import tpu as pltpu
from jax.sharding import Mesh
from jax.sharding import PartitionSpec as P

EXP_NODE = 10
PRESEL = 3
SRC_CAP = 16
LANES = 128
DP = ("dp_0", "dp_1", "dp_2")
NODE_DP = ("node", *DP)
TEAM = ("dp_0", "dp_2")
HALF = LANES // 2
PIECES = 3
OUT_PIECES = 4
F32 = jnp.float32
BF16 = jnp.bfloat16


def columns_of_routes(expert, slot, value):
    rows = []
    for c in range(PRESEL):
        named = (expert == c * EXP_NODE) & (slot >= 0)
        rows.append(jnp.sum(jnp.where(named, value, 0), axis=0, keepdims=True))
    return rows


def route_kernel(*refs):
    sources, out_ref, held, (send_ref, arrived, left) = refs[:5], refs[5], refs[6:11], refs[11:14]
    copies = [
        pltpu.make_async_copy(source, place, arrived.at[i])
        for i, (source, place) in enumerate(zip(sources, held))
    ]
    for copy in reversed(copies):
        copy.start()
    for copy in reversed(copies[1:]):
        copy.wait()
    og_ref, prob_ref, presel_ref, expert_ref, slot_ref = held
    tokens, features = og_ref.shape
    n_node = send_ref.shape[0] // SRC_CAP
    expert, slot, presel = expert_ref[...], slot_ref[...], presel_ref[...]
    slots = columns_of_routes(expert, slot, slot + 1)
    probs = columns_of_routes(expert, slot, prob_ref[...].astype(F32))
    node_ids = lax.broadcasted_iota(jnp.int32, (n_node, tokens), 0)
    slot_to = jnp.zeros((n_node, tokens), F32)
    prob_to = jnp.zeros((n_node, tokens), F32)
    for c in range(PRESEL):
        here = presel[c : c + 1] == node_ids
        slot_to += jnp.where(here, slots[c].astype(F32), 0.0)
        prob_to += jnp.where(here, probs[c], 0.0)
    sent = slot_to > 0.0
    before = lax.broadcasted_iota(jnp.int32, (tokens, tokens), 0) < lax.broadcasted_iota(
        jnp.int32, (tokens, tokens), 1
    )
    rank = jnp.dot(
        jnp.where(sent, 1.0, 0.0).astype(BF16),
        jnp.where(before, 1.0, 0.0).astype(BF16),
        preferred_element_type=F32,
    )
    rank = jnp.where(sent, rank, -1.0)
    place = lax.broadcasted_iota(jnp.int32, (n_node, SRC_CAP, tokens), 1).astype(F32)
    picked = rank[:, None, :] == place
    rows = n_node * SRC_CAP
    slot_rows = jnp.sum(jnp.where(picked, slot_to[:, None, :], 0.0), axis=2, keepdims=True)
    prob_rows = jnp.sum(jnp.where(picked, prob_to[:, None, :], 0.0), axis=2, keepdims=True)
    lane = lax.broadcasted_iota(jnp.int32, (n_node, SRC_CAP, LANES), 2)
    info = jnp.where(lane == 0, slot_rows, jnp.where(lane == 1, prob_rows, 0.0))
    send_ref[:, features:] = info.reshape(rows, LANES).astype(BF16)
    pick = jnp.where(picked, 1.0, 0.0).reshape(rows, tokens).astype(BF16)
    copies[0].wait()
    leaving = []
    piece = rows // OUT_PIECES
    for i in range(OUT_PIECES):
        some = slice(i * piece, (i + 1) * piece)
        send_ref[some, :features] = jnp.dot(
            pick[some], og_ref[...], preferred_element_type=F32
        ).astype(BF16)
        leaving.append(pltpu.make_async_copy(send_ref.at[some], out_ref.at[some], left.at[i]))
        leaving[-1].start()
    for copy in leaving:
        copy.wait()


def land_kernel(recv_ref, out_ref, scaled_ref, parts_ref, grad_p_ref):
    capacity, features = scaled_ref.shape
    recv = recv_ref[...]
    slot = recv_ref[:, features : features + 1].astype(F32)
    lane = lax.broadcasted_iota(jnp.int32, (recv.shape[0], LANES), 1).astype(F32)
    landing = jnp.where(slot == lane + 1.0, 1.0, 0.0).astype(BF16)
    landed = lax.dot_general(
        landing, recv, (((0,), (0,)), ((), ())), preferred_element_type=F32
    )[:capacity]
    dy = landed[:, :features]
    p = landed[:, features + 1 : features + 2]
    scaled = (p * dy).astype(BF16)
    scaled_ref[...] = scaled
    n = parts_ref.shape[0]
    rows = capacity // 2
    low = lax.broadcasted_iota(jnp.int32, (rows, LANES), 1) < HALF
    for k in range(n):
        for j in range(2):
            tile = 2 * k + j
            parts_ref[k, j * capacity : (j + 1) * capacity] = scaled[
                :, tile * LANES : (tile + 1) * LANES
            ]
    for k in range(n):
        tile = 2 * n + k // 2
        own = (p * dy[:, tile * LANES : (tile + 1) * LANES])
        swapped = pltpu.roll(own, HALF, 1)
        top, bottom = (own, swapped) if k % 2 == 0 else (swapped, own)
        parts_ref[k, 2 * capacity :] = jnp.where(low, top[:rows], bottom[rows:]).astype(BF16)
    grad_p = jnp.sum(dy * out_ref[...], axis=1, keepdims=True)
    row = lax.broadcasted_iota(jnp.int32, (capacity, LANES), 0)
    column = lax.broadcasted_iota(jnp.int32, (capacity, LANES), 1)
    grad_p_ref[...] = jnp.sum(jnp.where(row == column, grad_p, 0.0), axis=0, keepdims=True)


def collect_kernel(me_ref, *refs):
    *hidden_refs, out_ref, rows_ref = refs
    n_0 = len(hidden_refs)
    capacity = hidden_refs[0].shape[1]
    for k, hidden_ref in enumerate(hidden_refs):
        for j in range(2):
            block = lax.rem(me_ref[0] - k + n_0, n_0) * 2 + (me_ref[1] ^ j)
            start = pl.multiple_of(block * capacity, capacity)
            rows_ref[pl.ds(start, capacity)] = hidden_ref[j].astype(F32)
    out_ref[...] = rows_ref[...].T.astype(BF16)


def partial_kernel(hidden_ref, parts_ref, out_ref):
    team, rows, _ = parts_ref.shape
    capacity = rows * 2 // 5
    blocks = []
    for block in range(team):
        packed = parts_ref[block, 2 * capacity :].astype(F32)
        halves = jnp.concatenate([packed, pltpu.roll(packed, HALF, 1)]).astype(BF16)
        blocks.append(
            jnp.concatenate(
                [parts_ref[block, :capacity], parts_ref[block, capacity : 2 * capacity], halves],
                axis=1,
            )
        )
    total = jnp.dot(hidden_ref[...], jnp.concatenate(blocks), preferred_element_type=F32)
    n = out_ref.shape[0]
    share = total.shape[0] // n
    total = total.reshape(n, share, 3 * LANES)
    out_ref[:, :share] = total[:, :, :LANES].astype(BF16)
    out_ref[:, share : 2 * share] = total[:, :, LANES : 2 * LANES].astype(BF16)
    third = share // 3
    last = total[:, :, 2 * LANES :]
    low = lax.broadcasted_iota(jnp.int32, (n, third, LANES), 2) < HALF
    swapped = pltpu.roll(last[:, third : 2 * third], HALF, 2)
    mixed = jnp.where(low, last[:, :third], swapped)
    out_ref[:, 2 * share : 2 * share + third] = mixed.astype(BF16)
    out_ref[:, 2 * share + third :] = last[:, 2 * third :].astype(BF16)


def sum_kernel(n_0, n_1, terms_ref, out_ref):
    share = out_ref.shape[0]
    third = share // 3
    n = 2 * n_0
    low = lax.broadcasted_iota(jnp.int32, (third, LANES), 1) < HALF

    def put(row, tile, value):
        out_ref[row : row + value.shape[0], tile * LANES : (tile + 1) * LANES] = value.astype(BF16)

    for k in range(n_0):
        ends = []
        for j in range(2):
            total = None
            for i in range(n_1):
                term = terms_ref[(k * n_1 + i) * 2 + j].astype(F32)
                total = term if total is None else total + term
            tile = 2 * (2 * k + j)
            put(0, tile, total[:share])
            put(0, tile + 1, total[share : 2 * share])
            ends.append((total[2 * share : 2 * share + third], total[2 * share + third :]))
        (mixed_0, last_0), (mixed_1, last_1) = ends
        tile = 2 * n + k
        put(0, tile, jnp.where(low, mixed_0, pltpu.roll(mixed_1, HALF, 1)))
        put(third, tile, jnp.where(low, pltpu.roll(mixed_0, HALF, 1), mixed_1))
        put(2 * third, tile, jnp.where(low, last_0, pltpu.roll(last_1, HALF, 1)))


def grads_kernel(*refs):
    sources, grad_gate_ref, grad_up_ref = refs[:4], refs[4], refs[5]
    (scaled_ref, gate_ref, up_ref, weight_ref), arrived = refs[6:10], refs[10]
    copies = [
        pltpu.make_async_copy(source, place, arrived.at[i])
        for i, (source, place) in enumerate(zip(sources[:3], refs[6:9]))
    ]
    units = weight_ref.shape[0]
    piece = units // PIECES
    for i in range(PIECES):
        rows = pl.ds(i * piece, piece)
        copies.append(
            pltpu.make_async_copy(sources[3].at[rows], weight_ref.at[rows], arrived.at[3 + i])
        )
    for copy in copies:
        copy.start()
    for copy in copies[:3]:
        copy.wait()
    for i in range(PIECES):
        copies[3 + i].wait()
        rows = slice(i * piece, (i + 1) * piece)
        d_hidden = lax.dot_general(
            scaled_ref[...],
            weight_ref[rows],
            (((1,), (1,)), ((), ())),
            preferred_element_type=F32,
        )
        gate, up = gate_ref[:, rows].astype(F32), up_ref[:, rows].astype(F32)
        sigmoid = jax.nn.sigmoid(gate)
        slope = sigmoid * (1.0 + gate * (1.0 - sigmoid))
        grad_gate_ref[:, rows] = (d_hidden * up * slope).astype(BF16)
        grad_up_ref[:, rows] = (d_hidden * (gate * sigmoid)).astype(BF16)


def return_kernel(steps, me_ref, grad_p_ref, presel_ref, expert_ref, slot_ref, out_ref):
    n_node = grad_p_ref.shape[0]
    tokens = presel_ref.shape[1]
    expert, slot, presel = expert_ref[...], slot_ref[...], presel_ref[...]
    slots = columns_of_routes(expert, slot, slot + 1)
    row = lax.broadcasted_iota(jnp.int32, (n_node, tokens), 0)
    away = jnp.zeros((n_node, tokens), jnp.int32)
    for bit, step in enumerate(steps):
        away = jnp.where((row >> bit) & 1 == 1, away | step, away)
    slot_ids = lax.broadcasted_iota(jnp.int32, (LANES, tokens), 0)
    result = jnp.zeros(out_ref.shape, F32)
    for c in range(PRESEL):
        here = (presel[c : c + 1] ^ me_ref[0]) == away
        by_slot = lax.dot_general(
            grad_p_ref[...],
            jnp.where(here, 1.0, 0.0),
            (((0,), (0,)), ((), ())),
            preferred_element_type=F32,
            precision=lax.Precision.HIGHEST,
        )
        value = jnp.sum(jnp.where(slot_ids + 1 == slots[c], by_slot, 0.0), axis=0, keepdims=True)
        result += jnp.where((expert == c * EXP_NODE) & (slot >= 0), value, 0.0)
    out_ref[...] = result


HBM = pl.BlockSpec(memory_space=pltpu.HBM)
VMEM = pl.BlockSpec(memory_space=pltpu.VMEM)
SMEM = pl.BlockSpec(memory_space=pltpu.SMEM)


def call(kernel, out_shape, in_specs, scratch=(), vmem_mib=12, out_space=VMEM):
    many = isinstance(out_shape, (tuple, list))
    return pl.pallas_call(
        kernel,
        out_shape=out_shape,
        in_specs=in_specs,
        out_specs=[out_space] * len(out_shape) if many else out_space,
        scratch_shapes=scratch,
        compiler_params=pltpu.CompilerParams(vmem_limit_bytes=vmem_mib << 20),
    )


def exchange(value, axes):
    return lax.all_to_all(value, axes, split_axis=0, concat_axis=0, tiled=True)


def step_of(
    out_grad, gate_prob, presel_nodes, route_expert, route_slot, gate_pre, up_pre, down_weight
):
    _, features = out_grad.shape
    capacity, units = gate_pre.shape
    n_node, n_0, n_1, n_2 = (lax.axis_size(a) for a in NODE_DP)
    team = n_0 * n_2
    group = team * n_1
    share = units // group
    shape = jax.ShapeDtypeStruct
    presel, expert, slot = presel_nodes.T, route_expert.T, route_slot.T
    routed = (out_grad, gate_prob.T, presel, expert, slot)

    send = call(
        route_kernel,
        shape((n_node * SRC_CAP, features + LANES), BF16),
        [HBM] * 5,
        [pltpu.VMEM(a.shape, a.dtype) for a in routed]
        + [pltpu.VMEM((n_node * SRC_CAP, features + LANES), BF16)]
        + [pltpu.SemaphoreType.DMA((5,)), pltpu.SemaphoreType.DMA((OUT_PIECES,))],
        out_space=HBM,
        vmem_mib=60,
    )(*routed)
    recv = exchange(send.reshape(n_node, SRC_CAP, features + LANES), "node")
    recv = recv.reshape(n_node * SRC_CAP, features + LANES)

    weight = down_weight[0]
    gate_rows = gate_pre.astype(F32)
    up_rows = up_pre.astype(F32)
    sigmoid_gate = jax.nn.sigmoid(gate_rows)
    activated = gate_rows * sigmoid_gate
    hidden = (activated * up_rows).astype(BF16)
    near = lax.ppermute(hidden, "dp_2", [(0, 1), (1, 0)])
    hidden_pair = jnp.stack([hidden, near])
    hiddens = [hidden_pair]
    for k in range(1, n_0):
        hiddens.append(lax.ppermute(hidden_pair, "dp_0", [(i, (i + k) % n_0) for i in range(n_0)]))
    team_hidden = call(
        collect_kernel,
        shape((units, team * capacity), BF16),
        [SMEM] + [VMEM] * n_0,
        [pltpu.VMEM((team * capacity, units), F32)],
    )(jnp.stack([lax.axis_index(a) for a in TEAM]), *hiddens)
    slot_out = jnp.dot(hidden, weight, preferred_element_type=F32)

    scaled, parts, grad_p = call(
        land_kernel,
        [
            pltpu.HBM((capacity, features), BF16),
            pltpu.HBM((team, features * capacity // (team * LANES), LANES), BF16),
            shape((1, LANES), F32),
        ],
        [VMEM] * 2,
    )(recv, slot_out)
    parts = exchange(parts, TEAM)

    sources = (scaled, gate_pre, up_pre, weight)
    grad_gate, grad_up = call(
        grads_kernel,
        [shape((capacity, units), BF16)] * 2,
        [HBM] * 4,
        [pltpu.VMEM(a.shape, a.dtype) for a in sources]
        + [pltpu.SemaphoreType.DMA((3 + PIECES,))],
        vmem_mib=60,
    )(*sources)

    partial = call(
        partial_kernel, shape((group, 2 * share + 2 * share // 3, LANES), BF16), [VMEM] * 2
    )(team_hidden, parts)
    terms = exchange(partial, DP)
    grad_down = call(
        functools.partial(sum_kernel, n_0, n_1), shape((share, features), BF16), [VMEM]
    )(terms)[None]

    steps = [n_node >> (i + 1) for i in range(n_node.bit_length() - 1)]
    for step in steps:
        other = lax.ppermute(grad_p, "node", [(i, i ^ step) for i in range(n_node)])
        grad_p = jnp.concatenate([grad_p, other])
    grad_prob = call(
        functools.partial(return_kernel, steps),
        shape(route_expert.shape[::-1], F32),
        [SMEM] + [VMEM] * 4,
    )(lax.axis_index("node")[None], grad_p, presel, expert, slot).T
    return (grad_gate, grad_up, grad_down, grad_prob)


def solution(mesh):
    finer = Mesh(mesh.devices.reshape(mesh.shape["node"], 4, 4, 2), NODE_DP)
    in_specs = (P(NODE_DP, None),) * 7 + (P("node", None, None),)
    out_specs = (
        P(NODE_DP, None),
        P(NODE_DP, None),
        P("node", DP, None),
        P(NODE_DP, None),
    )
    return jax.shard_map(
        step_of, mesh=finer, in_specs=in_specs, out_specs=out_specs, check_vma=False
    )
```

```python
import functools

import jax
import jax.numpy as jnp
from jax import lax
from jax.experimental import pallas as pl
from jax.experimental.pallas import tpu as pltpu
from jax.sharding import Mesh
from jax.sharding import PartitionSpec as P

EXP_NODE = 10
PRESEL = 3
SRC_CAP = 16
LANES = 128
DP = ("dp_0", "dp_1", "dp_2")
NODE_DP = ("node", *DP)
TEAM = ("dp_0", "dp_2")
HALF = LANES // 2
PIECES = 3
OUT_PIECES = 4
F32 = jnp.float32
BF16 = jnp.bfloat16


def columns_of_routes(expert, slot, value):
    rows = []
    for c in range(PRESEL):
        named = (expert == c * EXP_NODE) & (slot >= 0)
        rows.append(jnp.sum(jnp.where(named, value, 0), axis=0, keepdims=True))
    return rows


def route_kernel(*refs):
    sources, out_ref, held, (send_ref, arrived, left) = refs[:5], refs[5], refs[6:11], refs[11:14]
    copies = [
        pltpu.make_async_copy(source, place, arrived.at[i])
        for i, (source, place) in enumerate(zip(sources, held))
    ]
    for copy in reversed(copies):
        copy.start()
    for copy in reversed(copies[1:]):
        copy.wait()
    og_ref, prob_ref, presel_ref, expert_ref, slot_ref = held
    tokens, features = og_ref.shape
    n_node = send_ref.shape[0] // SRC_CAP
    expert, slot, presel = expert_ref[...], slot_ref[...], presel_ref[...]
    slots = columns_of_routes(expert, slot, slot + 1)
    probs = columns_of_routes(expert, slot, prob_ref[...].astype(F32))
    node_ids = lax.broadcasted_iota(jnp.int32, (n_node, tokens), 0)
    slot_to = jnp.zeros((n_node, tokens), F32)
    prob_to = jnp.zeros((n_node, tokens), F32)
    for c in range(PRESEL):
        here = presel[c : c + 1] == node_ids
        slot_to += jnp.where(here, slots[c].astype(F32), 0.0)
        prob_to += jnp.where(here, probs[c], 0.0)
    sent = slot_to > 0.0
    before = lax.broadcasted_iota(jnp.int32, (tokens, tokens), 0) < lax.broadcasted_iota(
        jnp.int32, (tokens, tokens), 1
    )
    rank = jnp.dot(
        jnp.where(sent, 1.0, 0.0).astype(BF16),
        jnp.where(before, 1.0, 0.0).astype(BF16),
        preferred_element_type=F32,
    )
    rank = jnp.where(sent, rank, -1.0)
    place = lax.broadcasted_iota(jnp.int32, (n_node, SRC_CAP, tokens), 1).astype(F32)
    picked = rank[:, None, :] == place
    rows = n_node * SRC_CAP
    slot_rows = jnp.sum(jnp.where(picked, slot_to[:, None, :], 0.0), axis=2, keepdims=True)
    prob_rows = jnp.sum(jnp.where(picked, prob_to[:, None, :], 0.0), axis=2, keepdims=True)
    lane = lax.broadcasted_iota(jnp.int32, (n_node, SRC_CAP, LANES), 2)
    info = jnp.where(lane == 0, slot_rows, jnp.where(lane == 1, prob_rows, 0.0))
    send_ref[:, features:] = info.reshape(rows, LANES).astype(BF16)
    pick = jnp.where(picked, 1.0, 0.0).reshape(rows, tokens).astype(BF16)
    copies[0].wait()
    leaving = []
    piece = rows // OUT_PIECES
    for i in range(OUT_PIECES):
        some = slice(i * piece, (i + 1) * piece)
        send_ref[some, :features] = jnp.dot(
            pick[some], og_ref[...], preferred_element_type=F32
        ).astype(BF16)
        leaving.append(pltpu.make_async_copy(send_ref.at[some], out_ref.at[some], left.at[i]))
        leaving[-1].start()
    for copy in leaving:
        copy.wait()


def land_kernel(
    recv_ref, slot_out_ref, scaled_out_ref, out_ref, grad_p_ref, scaled_ref, parts_ref, left
):
    capacity, features = scaled_ref.shape
    recv = recv_ref[...]
    slot = recv_ref[:, features : features + 1].astype(F32)
    lane = lax.broadcasted_iota(jnp.int32, (recv.shape[0], LANES), 1).astype(F32)
    landing = jnp.where(slot == lane + 1.0, 1.0, 0.0).astype(BF16)
    landed = lax.dot_general(
        landing, recv, (((0,), (0,)), ((), ())), preferred_element_type=F32
    )[:capacity]
    dy = landed[:, :features]
    p = landed[:, features + 1 : features + 2]
    n = parts_ref.shape[0]
    rows = capacity // 2
    low = lax.broadcasted_iota(jnp.int32, (rows, LANES), 1) < HALF
    copies = []
    for k in range(n):
        for j in range(2):
            tile = slice((2 * k + j) * LANES, (2 * k + j + 1) * LANES)
            value = (p * dy[:, tile]).astype(BF16)
            scaled_ref[:, tile] = value
            parts_ref[k, j * capacity : (j + 1) * capacity] = value
        tile = slice((2 * n + k // 2) * LANES, (2 * n + k // 2 + 1) * LANES)
        own = p * dy[:, tile]
        if k % 2 == 0:
            scaled_ref[:, tile] = own.astype(BF16)
        swapped = pltpu.roll(own, HALF, 1)
        top, bottom = (own, swapped) if k % 2 == 0 else (swapped, own)
        parts_ref[k, 2 * capacity :] = jnp.where(low, top[:rows], bottom[rows:]).astype(BF16)
        copies.append(pltpu.make_async_copy(parts_ref.at[k], out_ref.at[k], left.at[k]))
        copies[-1].start()
    copies.append(pltpu.make_async_copy(scaled_ref, scaled_out_ref, left.at[n]))
    copies[-1].start()
    grad_p = jnp.sum(dy * slot_out_ref[...], axis=1, keepdims=True)
    row = lax.broadcasted_iota(jnp.int32, (capacity, LANES), 0)
    column = lax.broadcasted_iota(jnp.int32, (capacity, LANES), 1)
    grad_p_ref[...] = jnp.sum(jnp.where(row == column, grad_p, 0.0), axis=0, keepdims=True)
    for copy in copies:
        copy.wait()


def collect_kernel(me_ref, *refs):
    *hidden_refs, out_ref, rows_ref = refs
    n_0 = len(hidden_refs)
    capacity = hidden_refs[0].shape[1]
    for k, hidden_ref in enumerate(hidden_refs):
        for j in range(2):
            block = lax.rem(me_ref[0] - k + n_0, n_0) * 2 + (me_ref[1] ^ j)
            start = pl.multiple_of(block * capacity, capacity)
            rows_ref[pl.ds(start, capacity)] = hidden_ref[j].astype(F32)
    out_ref[...] = rows_ref[...].T.astype(BF16)


def partial_kernel(hidden_ref, parts_ref, out_ref, send_ref, left):
    team, rows, _ = parts_ref.shape
    capacity = rows * 2 // 5
    blocks = []
    for block in range(team):
        packed = parts_ref[block, 2 * capacity :].astype(F32)
        halves = jnp.concatenate([packed, pltpu.roll(packed, HALF, 1)]).astype(BF16)
        blocks.append(
            jnp.concatenate(
                [parts_ref[block, :capacity], parts_ref[block, capacity : 2 * capacity], halves],
                axis=1,
            )
        )
    scaled = jnp.concatenate(blocks)
    n = send_ref.shape[0]
    share = hidden_ref.shape[0] // n
    third = share // 3
    some = n // OUT_PIECES
    low = lax.broadcasted_iota(jnp.int32, (some, third, LANES), 2) < HALF
    copies = []
    for i in range(OUT_PIECES):
        here = slice(i * some, (i + 1) * some)
        total = jnp.dot(
            hidden_ref[i * some * share : (i + 1) * some * share],
            scaled,
            preferred_element_type=F32,
        ).reshape(some, share, 3 * LANES)
        send_ref[here, :share] = total[:, :, :LANES].astype(BF16)
        send_ref[here, share : 2 * share] = total[:, :, LANES : 2 * LANES].astype(BF16)
        last = total[:, :, 2 * LANES :]
        swapped = pltpu.roll(last[:, third : 2 * third], HALF, 2)
        mixed = jnp.where(low, last[:, :third], swapped)
        send_ref[here, 2 * share : 2 * share + third] = mixed.astype(BF16)
        send_ref[here, 2 * share + third :] = last[:, 2 * third :].astype(BF16)
        copies.append(pltpu.make_async_copy(send_ref.at[here], out_ref.at[here], left.at[i]))
        copies[-1].start()
    for copy in copies:
        copy.wait()


def sum_kernel(n_0, n_1, terms_ref, out_ref):
    share = out_ref.shape[0]
    third = share // 3
    n = 2 * n_0
    low = lax.broadcasted_iota(jnp.int32, (third, LANES), 1) < HALF

    def put(row, tile, value):
        out_ref[row : row + value.shape[0], tile * LANES : (tile + 1) * LANES] = value.astype(BF16)

    for k in range(n_0):
        ends = []
        for j in range(2):
            total = None
            for i in range(n_1):
                term = terms_ref[(k * n_1 + i) * 2 + j].astype(F32)
                total = term if total is None else total + term
            tile = 2 * (2 * k + j)
            put(0, tile, total[:share])
            put(0, tile + 1, total[share : 2 * share])
            ends.append((total[2 * share : 2 * share + third], total[2 * share + third :]))
        (mixed_0, last_0), (mixed_1, last_1) = ends
        tile = 2 * n + k
        put(0, tile, jnp.where(low, mixed_0, pltpu.roll(mixed_1, HALF, 1)))
        put(third, tile, jnp.where(low, pltpu.roll(mixed_0, HALF, 1), mixed_1))
        put(2 * third, tile, jnp.where(low, last_0, pltpu.roll(last_1, HALF, 1)))


def grads_kernel(*refs):
    sources, grad_gate_ref, grad_up_ref = refs[:4], refs[4], refs[5]
    (scaled_ref, gate_ref, up_ref, weight_ref), arrived = refs[6:10], refs[10]
    copies = [
        pltpu.make_async_copy(source, place, arrived.at[i])
        for i, (source, place) in enumerate(zip(sources[:3], refs[6:9]))
    ]
    units = weight_ref.shape[0]
    piece = units // PIECES
    for i in range(PIECES):
        rows = pl.ds(i * piece, piece)
        copies.append(
            pltpu.make_async_copy(sources[3].at[rows], weight_ref.at[rows], arrived.at[3 + i])
        )
    for copy in copies:
        copy.start()
    for copy in copies[:3]:
        copy.wait()
    for i in range(PIECES):
        copies[3 + i].wait()
        rows = slice(i * piece, (i + 1) * piece)
        d_hidden = lax.dot_general(
            scaled_ref[...],
            weight_ref[rows],
            (((1,), (1,)), ((), ())),
            preferred_element_type=F32,
        )
        gate, up = gate_ref[:, rows].astype(F32), up_ref[:, rows].astype(F32)
        sigmoid = jax.nn.sigmoid(gate)
        slope = sigmoid * (1.0 + gate * (1.0 - sigmoid))
        grad_gate_ref[:, rows] = (d_hidden * up * slope).astype(BF16)
        grad_up_ref[:, rows] = (d_hidden * (gate * sigmoid)).astype(BF16)


def return_kernel(steps, me_ref, grad_p_ref, presel_ref, expert_ref, slot_ref, out_ref):
    n_node = grad_p_ref.shape[0]
    tokens = presel_ref.shape[1]
    expert, slot, presel = expert_ref[...], slot_ref[...], presel_ref[...]
    slots = columns_of_routes(expert, slot, slot + 1)
    row = lax.broadcasted_iota(jnp.int32, (n_node, tokens), 0)
    away = jnp.zeros((n_node, tokens), jnp.int32)
    for bit, step in enumerate(steps):
        away = jnp.where((row >> bit) & 1 == 1, away | step, away)
    slot_ids = lax.broadcasted_iota(jnp.int32, (LANES, tokens), 0)
    result = jnp.zeros(out_ref.shape, F32)
    for c in range(PRESEL):
        here = (presel[c : c + 1] ^ me_ref[0]) == away
        by_slot = lax.dot_general(
            grad_p_ref[...],
            jnp.where(here, 1.0, 0.0),
            (((0,), (0,)), ((), ())),
            preferred_element_type=F32,
            precision=lax.Precision.HIGHEST,
        )
        value = jnp.sum(jnp.where(slot_ids + 1 == slots[c], by_slot, 0.0), axis=0, keepdims=True)
        result += jnp.where((expert == c * EXP_NODE) & (slot >= 0), value, 0.0)
    out_ref[...] = result


HBM = pl.BlockSpec(memory_space=pltpu.HBM)
VMEM = pl.BlockSpec(memory_space=pltpu.VMEM)
SMEM = pl.BlockSpec(memory_space=pltpu.SMEM)


def call(kernel, out_shape, in_specs, scratch=(), vmem_mib=12, out_space=VMEM):
    many = isinstance(out_shape, (tuple, list))
    return pl.pallas_call(
        kernel,
        out_shape=out_shape,
        in_specs=in_specs,
        out_specs=[out_space] * len(out_shape) if many and out_space is VMEM else out_space,
        scratch_shapes=scratch,
        compiler_params=pltpu.CompilerParams(vmem_limit_bytes=vmem_mib << 20),
    )


def exchange(value, axes):
    return lax.all_to_all(value, axes, split_axis=0, concat_axis=0, tiled=True)


def step_of(
    out_grad, gate_prob, presel_nodes, route_expert, route_slot, gate_pre, up_pre, down_weight
):
    _, features = out_grad.shape
    capacity, units = gate_pre.shape
    n_node, n_0, n_1, n_2 = (lax.axis_size(a) for a in NODE_DP)
    team = n_0 * n_2
    group = team * n_1
    share = units // group
    shape = jax.ShapeDtypeStruct
    presel, expert, slot = presel_nodes.T, route_expert.T, route_slot.T
    routed = (out_grad, gate_prob.T, presel, expert, slot)

    send = call(
        route_kernel,
        shape((n_node * SRC_CAP, features + LANES), BF16),
        [HBM] * 5,
        [pltpu.VMEM(a.shape, a.dtype) for a in routed]
        + [pltpu.VMEM((n_node * SRC_CAP, features + LANES), BF16)]
        + [pltpu.SemaphoreType.DMA((5,)), pltpu.SemaphoreType.DMA((OUT_PIECES,))],
        out_space=HBM,
        vmem_mib=60,
    )(*routed)
    recv = exchange(send.reshape(n_node, SRC_CAP, features + LANES), "node")
    recv = recv.reshape(n_node * SRC_CAP, features + LANES)

    weight = down_weight[0]
    gate_rows = gate_pre.astype(F32)
    hidden = (gate_rows * jax.nn.sigmoid(gate_rows) * up_pre.astype(F32)).astype(BF16)
    near = lax.ppermute(hidden, "dp_2", [(0, 1), (1, 0)])
    hidden_pair = jnp.stack([hidden, near])
    hiddens = [hidden_pair]
    for k in range(1, n_0):
        hiddens.append(lax.ppermute(hidden_pair, "dp_0", [(i, (i + k) % n_0) for i in range(n_0)]))
    team_hidden = call(
        collect_kernel,
        shape((units, team * capacity), BF16),
        [SMEM] + [VMEM] * n_0,
        [pltpu.VMEM((team * capacity, units), F32)],
    )(jnp.stack([lax.axis_index(a) for a in TEAM]), *hiddens)
    slot_out = jnp.dot(hidden, weight, preferred_element_type=F32)

    part = (team, features * capacity // (team * LANES), LANES)
    scaled, parts, grad_p = call(
        land_kernel,
        [
            pltpu.HBM((capacity, features), BF16),
            pltpu.HBM(part, BF16),
            pltpu.VMEM((1, LANES), F32),
        ],
        [VMEM] * 2,
        [
            pltpu.VMEM((capacity, features), BF16),
            pltpu.VMEM(part, BF16),
            pltpu.SemaphoreType.DMA((1 + team,)),
        ],
        out_space=[HBM, HBM, VMEM],
    )(recv, slot_out)
    parts = exchange(parts, TEAM)

    sources = (scaled, gate_pre, up_pre, weight)
    grad_gate, grad_up = call(
        grads_kernel,
        [shape((capacity, units), BF16)] * 2,
        [HBM] * 4,
        [pltpu.VMEM(a.shape, a.dtype) for a in sources]
        + [pltpu.SemaphoreType.DMA((3 + PIECES,))],
        vmem_mib=60,
    )(*sources)

    terms = (group, 2 * share + 2 * share // 3, LANES)
    partial = call(
        partial_kernel,
        pltpu.HBM(terms, BF16),
        [VMEM] * 2,
        [pltpu.VMEM(terms, BF16), pltpu.SemaphoreType.DMA((OUT_PIECES,))],
        out_space=HBM,
    )(team_hidden, parts)
    terms = exchange(partial, DP)
    grad_down = call(
        functools.partial(sum_kernel, n_0, n_1), shape((share, features), BF16), [VMEM]
    )(terms)[None]

    steps = [n_node >> (i + 1) for i in range(n_node.bit_length() - 1)]
    for step in steps:
        other = lax.ppermute(grad_p, "node", [(i, i ^ step) for i in range(n_node)])
        grad_p = jnp.concatenate([grad_p, other])
    grad_prob = call(
        functools.partial(return_kernel, steps),
        shape(route_expert.shape[::-1], F32),
        [SMEM] + [VMEM] * 4,
    )(lax.axis_index("node")[None], grad_p, presel, expert, slot).T
    return (grad_gate, grad_up, grad_down, grad_prob)


def solution(mesh):
    finer = Mesh(mesh.devices.reshape(mesh.shape["node"], 4, 4, 2), NODE_DP)
    in_specs = (P(NODE_DP, None),) * 7 + (P("node", None, None),)
    out_specs = (
        P(NODE_DP, None),
        P(NODE_DP, None),
        P("node", DP, None),
        P(NODE_DP, None),
    )
    return jax.shard_map(
        step_of, mesh=finer, in_specs=in_specs, out_specs=out_specs, check_vma=False
    )
```

```python
import functools

import jax
import jax.numpy as jnp
from jax import lax
from jax.experimental import pallas as pl
from jax.experimental.pallas import tpu as pltpu
from jax.sharding import Mesh
from jax.sharding import PartitionSpec as P

EXP_NODE = 10
PRESEL = 3
SRC_CAP = 16
LANES = 128
DP = ("dp_0", "dp_1", "dp_2")
NODE_DP = ("node", *DP)
TEAM = ("dp_0", "dp_2")
HALF = LANES // 2
OUT_PIECES = 4
F32 = jnp.float32
BF16 = jnp.bfloat16


def columns_of_routes(expert, slot, value):
    rows = []
    for c in range(PRESEL):
        named = (expert == c * EXP_NODE) & (slot >= 0)
        rows.append(jnp.sum(jnp.where(named, value, 0), axis=0, keepdims=True))
    return rows


def route_kernel(*refs):
    sources, out_ref, held, (send_ref, arrived, left) = refs[:5], refs[5], refs[6:11], refs[11:14]
    copies = [
        pltpu.make_async_copy(source, place, arrived.at[i])
        for i, (source, place) in enumerate(zip(sources, held))
    ]
    for copy in reversed(copies):
        copy.start()
    for copy in reversed(copies[1:]):
        copy.wait()
    og_ref, prob_ref, presel_ref, expert_ref, slot_ref = held
    tokens, features = og_ref.shape
    n_node = send_ref.shape[0]
    expert, slot, presel = expert_ref[...], slot_ref[...], presel_ref[...]
    slots = columns_of_routes(expert, slot, slot + 1)
    probs = columns_of_routes(expert, slot, prob_ref[...].astype(F32))
    node_ids = lax.broadcasted_iota(jnp.int32, (n_node, tokens), 0)
    slot_to = jnp.zeros((n_node, tokens), F32)
    prob_to = jnp.zeros((n_node, tokens), F32)
    for c in range(PRESEL):
        here = presel[c : c + 1] == node_ids
        slot_to += jnp.where(here, slots[c].astype(F32), 0.0)
        prob_to += jnp.where(here, probs[c], 0.0)
    sent = slot_to > 0.0
    before = lax.broadcasted_iota(jnp.int32, (tokens, tokens), 0) < lax.broadcasted_iota(
        jnp.int32, (tokens, tokens), 1
    )
    rank = jnp.dot(
        jnp.where(sent, 1.0, 0.0).astype(BF16),
        jnp.where(before, 1.0, 0.0).astype(BF16),
        preferred_element_type=F32,
    )
    rank = jnp.where(sent, rank, -1.0)
    place = lax.broadcasted_iota(jnp.int32, (n_node, SRC_CAP, tokens), 1).astype(F32)
    picked = rank[:, None, :] == place
    rows = n_node * SRC_CAP
    slot_rows = jnp.sum(jnp.where(picked, slot_to[:, None, :], 0.0), axis=2, keepdims=True)
    prob_rows = jnp.sum(jnp.where(picked, prob_to[:, None, :], 0.0), axis=2, keepdims=True)
    half = SRC_CAP // 2
    lane = lax.broadcasted_iota(jnp.int32, (n_node, half, LANES), 2)
    info = jnp.zeros((n_node, half, LANES), F32)
    for i, column in enumerate(
        (slot_rows[:, :half], prob_rows[:, :half], slot_rows[:, half:], prob_rows[:, half:])
    ):
        info = jnp.where(lane == i, column, info)
    tiles = features // LANES
    send_ref[:, tiles * SRC_CAP :] = info.astype(BF16)
    pick = jnp.where(picked, 1.0, 0.0).reshape(rows, tokens).astype(BF16)
    copies[0].wait()
    leaving = []
    some = n_node // OUT_PIECES
    for i in range(OUT_PIECES):
        here = slice(i * some, (i + 1) * some)
        taken = jnp.dot(
            pick[i * some * SRC_CAP : (i + 1) * some * SRC_CAP],
            og_ref[...],
            preferred_element_type=F32,
        )
        for k in range(tiles):
            send_ref[here, k * SRC_CAP : (k + 1) * SRC_CAP] = (
                taken[:, k * LANES : (k + 1) * LANES].reshape(some, SRC_CAP, LANES).astype(BF16)
            )
        leaving.append(pltpu.make_async_copy(send_ref.at[here], out_ref.at[here], left.at[i]))
        leaving[-1].start()
    for copy in leaving:
        copy.wait()


def land_kernel(
    recv_ref, slot_out_ref, scaled_out_ref, out_ref, grad_p_ref, scaled_ref, parts_ref, left
):
    capacity, features = scaled_ref.shape
    n_node = recv_ref.shape[0]
    rows = n_node * SRC_CAP
    info = recv_ref[:, features // LANES * SRC_CAP :].astype(F32)
    slot, prob = (
        jnp.concatenate([info[:, :, i : i + 1], info[:, :, i + 2 : i + 3]], axis=1).reshape(rows, 1)
        for i in range(2)
    )
    lane = lax.broadcasted_iota(jnp.int32, (rows, LANES), 1).astype(F32)
    landing = jnp.where(slot == lane + 1.0, 1.0, 0.0).T[:capacity].astype(BF16)

    def landed(value):
        return jnp.dot(landing, value, preferred_element_type=F32)

    def pair(tile):
        return landed(
            jnp.concatenate(
                [
                    recv_ref[:, i * SRC_CAP : (i + 1) * SRC_CAP].reshape(rows, LANES)
                    for i in (tile, tile + 1)
                ],
                axis=1,
            )
        )

    p = landed(jnp.where(lane < LANES, prob, 0.0).astype(BF16))
    n = parts_ref.shape[0]
    half = capacity // 2
    low = lax.broadcasted_iota(jnp.int32, (half, LANES), 1) < HALF
    sums = jnp.zeros((capacity, LANES), F32)

    def settle(dy, tile):
        value = p * dy
        here = slice(tile * LANES, (tile + 1) * LANES)
        scaled_ref[:, here] = value.astype(BF16)
        return value, dy * slot_out_ref[:, here]

    for tile in range(2 * n, features // LANES, 2):
        both = pair(tile)
        for i in range(2):
            own, term = settle(both[:, i * LANES : (i + 1) * LANES], tile + i)
            sums += term
            k = 2 * (tile + i - 2 * n)
            swapped = pltpu.roll(own, HALF, 1)
            parts_ref[k, 2 * capacity :] = jnp.where(low, own[:half], swapped[half:]).astype(BF16)
            parts_ref[k + 1, 2 * capacity :] = jnp.where(low, swapped[:half], own[half:]).astype(
                BF16
            )
    copies = []
    for k in range(n):
        both = pair(2 * k)
        for j in range(2):
            own, term = settle(both[:, j * LANES : (j + 1) * LANES], 2 * k + j)
            sums += term
            parts_ref[k, j * capacity : (j + 1) * capacity] = own.astype(BF16)
        copies.append(pltpu.make_async_copy(parts_ref.at[k], out_ref.at[k], left.at[k]))
        copies[-1].start()
    copies.append(pltpu.make_async_copy(scaled_ref, scaled_out_ref, left.at[n]))
    copies[-1].start()
    grad_p = jnp.sum(sums, axis=1, keepdims=True)
    row = lax.broadcasted_iota(jnp.int32, (capacity, LANES), 0)
    column = lax.broadcasted_iota(jnp.int32, (capacity, LANES), 1)
    grad_p_ref[...] = jnp.sum(jnp.where(row == column, grad_p, 0.0), axis=0, keepdims=True)
    for copy in copies:
        copy.wait()


def collect_kernel(me_ref, *refs):
    *hidden_refs, out_ref, rows_ref = refs
    n_0 = len(hidden_refs)
    capacity = hidden_refs[0].shape[1]
    for k, hidden_ref in enumerate(hidden_refs):
        for j in range(2):
            block = lax.rem(me_ref[0] - k + n_0, n_0) * 2 + (me_ref[1] ^ j)
            start = pl.multiple_of(block * capacity, capacity)
            rows_ref[pl.ds(start, capacity)] = hidden_ref[j].astype(F32)
    out_ref[...] = rows_ref[...].T.astype(BF16)


def partial_kernel(hidden_ref, parts_ref, out_ref, send_ref, left):
    team, rows, _ = parts_ref.shape
    capacity = rows * 2 // 5
    blocks = []
    for block in range(team):
        packed = parts_ref[block, 2 * capacity :].astype(F32)
        halves = jnp.concatenate([packed, pltpu.roll(packed, HALF, 1)]).astype(BF16)
        blocks.append(
            jnp.concatenate(
                [parts_ref[block, :capacity], parts_ref[block, capacity : 2 * capacity], halves],
                axis=1,
            )
        )
    scaled = jnp.concatenate(blocks)
    n = send_ref.shape[0]
    share = hidden_ref.shape[0] // n
    third = share // 3
    some = n // OUT_PIECES
    low = lax.broadcasted_iota(jnp.int32, (some, third, LANES), 2) < HALF
    copies = []
    for i in range(OUT_PIECES):
        here = slice(i * some, (i + 1) * some)
        total = jnp.dot(
            hidden_ref[i * some * share : (i + 1) * some * share],
            scaled,
            preferred_element_type=F32,
        ).reshape(some, share, 3 * LANES)
        send_ref[here, :share] = total[:, :, :LANES].astype(BF16)
        send_ref[here, share : 2 * share] = total[:, :, LANES : 2 * LANES].astype(BF16)
        last = total[:, :, 2 * LANES :]
        swapped = pltpu.roll(last[:, third : 2 * third], HALF, 2)
        mixed = jnp.where(low, last[:, :third], swapped)
        send_ref[here, 2 * share : 2 * share + third] = mixed.astype(BF16)
        send_ref[here, 2 * share + third :] = last[:, 2 * third :].astype(BF16)
        copies.append(pltpu.make_async_copy(send_ref.at[here], out_ref.at[here], left.at[i]))
        copies[-1].start()
    for copy in copies:
        copy.wait()


def sum_kernel(n_0, n_1, terms_ref, out_ref):
    share = out_ref.shape[0]
    third = share // 3
    n = 2 * n_0
    low = lax.broadcasted_iota(jnp.int32, (third, LANES), 1) < HALF

    def put(row, tile, value):
        out_ref[row : row + value.shape[0], tile * LANES : (tile + 1) * LANES] = value.astype(BF16)

    for k in range(n_0):
        ends = []
        for j in range(2):
            total = None
            for i in range(n_1):
                term = terms_ref[(k * n_1 + i) * 2 + j].astype(F32)
                total = term if total is None else total + term
            tile = 2 * (2 * k + j)
            put(0, tile, total[:share])
            put(0, tile + 1, total[share : 2 * share])
            ends.append((total[2 * share : 2 * share + third], total[2 * share + third :]))
        (mixed_0, last_0), (mixed_1, last_1) = ends
        tile = 2 * n + k
        put(0, tile, jnp.where(low, mixed_0, pltpu.roll(mixed_1, HALF, 1)))
        put(third, tile, jnp.where(low, pltpu.roll(mixed_0, HALF, 1), mixed_1))
        put(2 * third, tile, jnp.where(low, last_0, pltpu.roll(last_1, HALF, 1)))


def grads_kernel(first, *refs):
    sources, (gate_out_ref, up_out_ref) = refs[:4], refs[-10:-8]
    scaled_ref, gate_ref, up_ref, weight_ref, gate_grad_ref, up_grad_ref = refs[-8:-2]
    arrived, left = [refs[-2].at[i] for i in range(5)], refs[-1]
    units = weight_ref.shape[0]
    piece = units // 2
    columns = pl.ds(first, units)
    copies = [
        pltpu.make_async_copy(sources[0], scaled_ref, arrived[0]),
        pltpu.make_async_copy(sources[1].at[:, columns], gate_ref, arrived[1]),
        pltpu.make_async_copy(sources[2].at[:, columns], up_ref, arrived[2]),
    ]
    for i in range(2):
        copies.append(
            pltpu.make_async_copy(
                sources[3].at[pl.ds(first + i * piece, piece)],
                weight_ref.at[pl.ds(i * piece, piece)],
                arrived[3 + i],
            )
        )
    for copy in copies:
        copy.start()
    for copy in copies[:3]:
        copy.wait()
    for i in range(2):
        copies[3 + i].wait()
        here = slice(i * piece, (i + 1) * piece)
        d_hidden = lax.dot_general(
            scaled_ref[...],
            weight_ref[here],
            (((1,), (1,)), ((), ())),
            preferred_element_type=F32,
        )
        gate, up = gate_ref[:, here].astype(F32), up_ref[:, here].astype(F32)
        sigmoid = jax.nn.sigmoid(gate)
        slope = sigmoid * (1.0 + gate * (1.0 - sigmoid))
        gate_grad_ref[:, here] = (d_hidden * up * slope).astype(BF16)
        up_grad_ref[:, here] = (d_hidden * (gate * sigmoid)).astype(BF16)
    copies = [
        pltpu.make_async_copy(gate_grad_ref, gate_out_ref.at[:, columns], left.at[0]),
        pltpu.make_async_copy(up_grad_ref, up_out_ref.at[:, columns], left.at[1]),
    ]
    for copy in copies:
        copy.start()
    for copy in copies:
        copy.wait()


def return_kernel(steps, me_ref, grad_p_ref, presel_ref, expert_ref, slot_ref, out_ref):
    n_node = grad_p_ref.shape[0]
    tokens = presel_ref.shape[1]
    expert, slot, presel = expert_ref[...], slot_ref[...], presel_ref[...]
    slots = columns_of_routes(expert, slot, slot + 1)
    row = lax.broadcasted_iota(jnp.int32, (n_node, tokens), 0)
    away = jnp.zeros((n_node, tokens), jnp.int32)
    for bit, step in enumerate(steps):
        away = jnp.where((row >> bit) & 1 == 1, away | step, away)
    slot_ids = lax.broadcasted_iota(jnp.int32, (LANES, tokens), 0)
    here = jnp.concatenate(
        [
            jnp.where((presel[c : c + 1] ^ me_ref[0]) == away, 1.0, 0.0)
            for c in range(PRESEL)
        ],
        axis=1,
    )
    by_slot = lax.dot_general(
        grad_p_ref[...],
        here,
        (((0,), (0,)), ((), ())),
        preferred_element_type=F32,
        precision=lax.Precision.HIGHEST,
    )
    result = jnp.zeros(out_ref.shape, F32)
    for c in range(PRESEL):
        values = by_slot[:, c * tokens : (c + 1) * tokens]
        value = jnp.sum(jnp.where(slot_ids + 1 == slots[c], values, 0.0), axis=0, keepdims=True)
        result += jnp.where((expert == c * EXP_NODE) & (slot >= 0), value, 0.0)
    out_ref[...] = result


HBM = pl.BlockSpec(memory_space=pltpu.HBM)
VMEM = pl.BlockSpec(memory_space=pltpu.VMEM)
SMEM = pl.BlockSpec(memory_space=pltpu.SMEM)


def call(kernel, out_shape, in_specs, scratch=(), vmem_mib=12, out_space=VMEM, aliases=None):
    many = isinstance(out_shape, (tuple, list))
    return pl.pallas_call(
        kernel,
        out_shape=out_shape,
        in_specs=in_specs,
        out_specs=[out_space] * len(out_shape)
        if many and not isinstance(out_space, list)
        else out_space,
        scratch_shapes=scratch,
        input_output_aliases=aliases or {},
        compiler_params=pltpu.CompilerParams(vmem_limit_bytes=vmem_mib << 20),
    )


def exchange(value, axes):
    return lax.all_to_all(value, axes, split_axis=0, concat_axis=0, tiled=True)


def step_of(
    out_grad, gate_prob, presel_nodes, route_expert, route_slot, gate_pre, up_pre, down_weight
):
    _, features = out_grad.shape
    capacity, units = gate_pre.shape
    n_node, n_0, n_1, n_2 = (lax.axis_size(a) for a in NODE_DP)
    team = n_0 * n_2
    group = team * n_1
    share = units // group
    shape = jax.ShapeDtypeStruct
    presel, expert, slot = presel_nodes.T, route_expert.T, route_slot.T
    routed = (out_grad, gate_prob.T, presel, expert, slot)

    chunks = (n_node, features // LANES * SRC_CAP + SRC_CAP // 2, LANES)
    send = call(
        route_kernel,
        shape(chunks, BF16),
        [HBM] * 5,
        [pltpu.VMEM(a.shape, a.dtype) for a in routed]
        + [pltpu.VMEM(chunks, BF16)]
        + [pltpu.SemaphoreType.DMA((5,)), pltpu.SemaphoreType.DMA((OUT_PIECES,))],
        out_space=HBM,
        vmem_mib=60,
    )(*routed)
    recv = exchange(send, "node")

    weight = down_weight[0]
    gate_rows = gate_pre.astype(F32)
    hidden = (gate_rows * jax.nn.sigmoid(gate_rows) * up_pre.astype(F32)).astype(BF16)
    near = lax.ppermute(hidden, "dp_2", [(0, 1), (1, 0)])
    hidden_pair = jnp.stack([hidden, near])
    hiddens = [hidden_pair]
    for k in range(1, n_0):
        hiddens.append(lax.ppermute(hidden_pair, "dp_0", [(i, (i + k) % n_0) for i in range(n_0)]))
    team_hidden = call(
        collect_kernel,
        shape((units, team * capacity), BF16),
        [SMEM] + [VMEM] * n_0,
        [pltpu.VMEM((team * capacity, units), F32)],
    )(jnp.stack([lax.axis_index(a) for a in TEAM]), *hiddens)
    slot_out = jnp.dot(hidden, weight, preferred_element_type=F32)

    part = (team, features * capacity // (team * LANES), LANES)
    scaled, parts, grad_p = call(
        land_kernel,
        [
            pltpu.HBM((capacity, features), BF16),
            pltpu.HBM(part, BF16),
            pltpu.VMEM((1, LANES), F32),
        ],
        [VMEM] * 2,
        [
            pltpu.VMEM((capacity, features), BF16),
            pltpu.VMEM(part, BF16),
            pltpu.SemaphoreType.DMA((1 + team,)),
        ],
        out_space=[HBM, HBM, VMEM],
    )(recv, slot_out)
    parts = exchange(parts, TEAM)

    sources = (scaled, gate_pre, up_pre, weight)
    piece = units // 2
    grads = ()
    for i in range(2):
        grads = call(
            functools.partial(grads_kernel, i * piece),
            [pltpu.HBM((capacity, units), BF16)] * 2,
            [HBM] * (4 + len(grads)),
            [pltpu.VMEM(scaled.shape, BF16)]
            + [pltpu.VMEM((capacity, piece), BF16)] * 2
            + [pltpu.VMEM((piece, features), BF16)]
            + [pltpu.VMEM((capacity, piece), BF16)] * 2
            + [pltpu.SemaphoreType.DMA((5,)), pltpu.SemaphoreType.DMA((2,))],
            vmem_mib=60,
            out_space=HBM,
            aliases={4 + k: k for k in range(len(grads))},
        )(*sources, *grads)
    grad_gate, grad_up = grads

    terms = (group, 2 * share + 2 * share // 3, LANES)
    partial = call(
        partial_kernel,
        pltpu.HBM(terms, BF16),
        [VMEM] * 2,
        [pltpu.VMEM(terms, BF16), pltpu.SemaphoreType.DMA((OUT_PIECES,))],
        out_space=HBM,
    )(team_hidden, parts)
    terms = exchange(partial, DP)
    grad_down = call(
        functools.partial(sum_kernel, n_0, n_1), shape((share, features), BF16), [VMEM]
    )(terms)[None]

    steps = [n_node >> (i + 1) for i in range(n_node.bit_length() - 1)]
    for step in steps:
        other = lax.ppermute(grad_p, "node", [(i, i ^ step) for i in range(n_node)])
        grad_p = jnp.concatenate([grad_p, other])
    grad_prob = call(
        functools.partial(return_kernel, steps),
        shape(route_expert.shape[::-1], F32),
        [SMEM] + [VMEM] * 4,
    )(lax.axis_index("node")[None], grad_p, presel, expert, slot).T
    return (grad_gate, grad_up, grad_down, grad_prob)


def solution(mesh):
    finer = Mesh(mesh.devices.reshape(mesh.shape["node"], 4, 4, 2), NODE_DP)
    in_specs = (P(NODE_DP, None),) * 7 + (P("node", None, None),)
    out_specs = (
        P(NODE_DP, None),
        P(NODE_DP, None),
        P("node", DP, None),
        P(NODE_DP, None),
    )
    return jax.shard_map(
        step_of, mesh=finer, in_specs=in_specs, out_specs=out_specs, check_vma=False
    )
```

```python
import functools

import jax
import jax.numpy as jnp
from jax import lax
from jax.experimental import pallas as pl
from jax.experimental.pallas import tpu as pltpu
from jax.sharding import Mesh
from jax.sharding import PartitionSpec as P

EXP_NODE = 10
PRESEL = 3
SRC_CAP = 16
LANES = 128
DP = ("dp_0", "dp_1", "dp_2")
NODE_DP = ("node", *DP)
TEAM = ("dp_0", "dp_2")
HALF = LANES // 2
PIECES = 3
OUT_PIECES = 4
F32 = jnp.float32
BF16 = jnp.bfloat16


def columns_of_routes(expert, slot, value):
    rows = []
    for c in range(PRESEL):
        named = (expert == c * EXP_NODE) & (slot >= 0)
        rows.append(jnp.sum(jnp.where(named, value, 0), axis=0, keepdims=True))
    return rows


def route_kernel(*refs):
    sources, out_ref, held, (send_ref, arrived, left) = refs[:5], refs[5], refs[6:11], refs[11:14]
    copies = [
        pltpu.make_async_copy(source, place, arrived.at[i])
        for i, (source, place) in enumerate(zip(sources, held))
    ]
    for copy in reversed(copies):
        copy.start()
    for copy in reversed(copies[1:]):
        copy.wait()
    og_ref, prob_ref, presel_ref, expert_ref, slot_ref = held
    tokens, features = og_ref.shape
    n_node = send_ref.shape[0]
    expert, slot, presel = expert_ref[...], slot_ref[...], presel_ref[...]
    slots = columns_of_routes(expert, slot, slot + 1)
    probs = columns_of_routes(expert, slot, prob_ref[...].astype(F32))
    node_ids = lax.broadcasted_iota(jnp.int32, (n_node, tokens), 0)
    slot_to = jnp.zeros((n_node, tokens), F32)
    prob_to = jnp.zeros((n_node, tokens), F32)
    for c in range(PRESEL):
        here = presel[c : c + 1] == node_ids
        slot_to += jnp.where(here, slots[c].astype(F32), 0.0)
        prob_to += jnp.where(here, probs[c], 0.0)
    sent = slot_to > 0.0
    before = lax.broadcasted_iota(jnp.int32, (tokens, tokens), 0) < lax.broadcasted_iota(
        jnp.int32, (tokens, tokens), 1
    )
    rank = jnp.dot(
        jnp.where(sent, 1.0, 0.0).astype(BF16),
        jnp.where(before, 1.0, 0.0).astype(BF16),
        preferred_element_type=F32,
    )
    rank = jnp.where(sent, rank, -1.0)
    place = lax.broadcasted_iota(jnp.int32, (n_node, SRC_CAP, tokens), 1).astype(F32)
    picked = rank[:, None, :] == place
    rows = n_node * SRC_CAP
    slot_rows = jnp.sum(jnp.where(picked, slot_to[:, None, :], 0.0), axis=2, keepdims=True)
    prob_rows = jnp.sum(jnp.where(picked, prob_to[:, None, :], 0.0), axis=2, keepdims=True)
    half = SRC_CAP // 2
    lane = lax.broadcasted_iota(jnp.int32, (n_node, half, LANES), 2)
    info = jnp.zeros((n_node, half, LANES), F32)
    for i, column in enumerate(
        (slot_rows[:, :half], prob_rows[:, :half], slot_rows[:, half:], prob_rows[:, half:])
    ):
        info = jnp.where(lane == i, column, info)
    tiles = features // LANES
    send_ref[:, tiles * SRC_CAP :] = info.astype(BF16)
    pick = jnp.where(picked, 1.0, 0.0).reshape(rows, tokens).astype(BF16)
    copies[0].wait()
    leaving = []
    some = n_node // OUT_PIECES
    for i in range(OUT_PIECES):
        here = slice(i * some, (i + 1) * some)
        taken = jnp.dot(
            pick[i * some * SRC_CAP : (i + 1) * some * SRC_CAP],
            og_ref[...],
            preferred_element_type=F32,
        )
        for k in range(tiles):
            send_ref[here, k * SRC_CAP : (k + 1) * SRC_CAP] = (
                taken[:, k * LANES : (k + 1) * LANES].reshape(some, SRC_CAP, LANES).astype(BF16)
            )
        leaving.append(pltpu.make_async_copy(send_ref.at[here], out_ref.at[here], left.at[i]))
        leaving[-1].start()
    for copy in leaving:
        copy.wait()


def land_kernel(
    recv_ref, slot_out_ref, scaled_out_ref, out_ref, grad_p_ref, scaled_ref, parts_ref, left
):
    capacity, features = scaled_ref.shape
    n_node = recv_ref.shape[0]
    rows = n_node * SRC_CAP
    info = recv_ref[:, features // LANES * SRC_CAP :].astype(F32)
    slot, prob = (
        jnp.concatenate([info[:, :, i : i + 1], info[:, :, i + 2 : i + 3]], axis=1).reshape(rows, 1)
        for i in range(2)
    )
    lane = lax.broadcasted_iota(jnp.int32, (rows, LANES), 1).astype(F32)
    landing = jnp.where(slot == lane + 1.0, 1.0, 0.0).T[:capacity].astype(BF16)

    def landed(value):
        return jnp.dot(landing, value, preferred_element_type=F32)

    def pair(tile):
        return landed(
            jnp.concatenate(
                [
                    recv_ref[:, i * SRC_CAP : (i + 1) * SRC_CAP].reshape(rows, LANES)
                    for i in (tile, tile + 1)
                ],
                axis=1,
            )
        )

    p = landed(jnp.where(lane < LANES, prob, 0.0).astype(BF16))
    n = parts_ref.shape[0]
    half = capacity // 2
    low = lax.broadcasted_iota(jnp.int32, (half, LANES), 1) < HALF
    sums = jnp.zeros((capacity, LANES), F32)

    def settle(dy, tile):
        value = p * dy
        here = slice(tile * LANES, (tile + 1) * LANES)
        scaled_ref[:, here] = value.astype(BF16)
        return value, dy * slot_out_ref[:, here]

    for tile in range(2 * n, features // LANES, 2):
        both = pair(tile)
        for i in range(2):
            own, term = settle(both[:, i * LANES : (i + 1) * LANES], tile + i)
            sums += term
            k = 2 * (tile + i - 2 * n)
            swapped = pltpu.roll(own, HALF, 1)
            parts_ref[k, 2 * capacity :] = jnp.where(low, own[:half], swapped[half:]).astype(BF16)
            parts_ref[k + 1, 2 * capacity :] = jnp.where(low, swapped[:half], own[half:]).astype(
                BF16
            )
    copies = []
    for k in range(n):
        both = pair(2 * k)
        for j in range(2):
            own, term = settle(both[:, j * LANES : (j + 1) * LANES], 2 * k + j)
            sums += term
            parts_ref[k, j * capacity : (j + 1) * capacity] = own.astype(BF16)
        copies.append(pltpu.make_async_copy(parts_ref.at[k], out_ref.at[k], left.at[k]))
        copies[-1].start()
    copies.append(pltpu.make_async_copy(scaled_ref, scaled_out_ref, left.at[n]))
    copies[-1].start()
    grad_p = jnp.sum(sums, axis=1, keepdims=True)
    row = lax.broadcasted_iota(jnp.int32, (capacity, LANES), 0)
    column = lax.broadcasted_iota(jnp.int32, (capacity, LANES), 1)
    grad_p_ref[...] = jnp.sum(jnp.where(row == column, grad_p, 0.0), axis=0, keepdims=True)
    for copy in copies:
        copy.wait()


def collect_kernel(me_ref, *refs):
    *hidden_refs, out_ref, rows_ref = refs
    n_0 = len(hidden_refs)
    capacity = hidden_refs[0].shape[1]
    for k, hidden_ref in enumerate(hidden_refs):
        for j in range(2):
            block = lax.rem(me_ref[0] - k + n_0, n_0) * 2 + (me_ref[1] ^ j)
            start = pl.multiple_of(block * capacity, capacity)
            rows_ref[pl.ds(start, capacity)] = hidden_ref[j].astype(F32)
    out_ref[...] = rows_ref[...].T.astype(BF16)


def partial_kernel(hidden_ref, parts_ref, out_ref, send_ref, left):
    team, rows, _ = parts_ref.shape
    capacity = rows * 2 // 5
    blocks = []
    for block in range(team):
        packed = parts_ref[block, 2 * capacity :].astype(F32)
        halves = jnp.concatenate([packed, pltpu.roll(packed, HALF, 1)]).astype(BF16)
        blocks.append(
            jnp.concatenate(
                [parts_ref[block, :capacity], parts_ref[block, capacity : 2 * capacity], halves],
                axis=1,
            )
        )
    scaled = jnp.concatenate(blocks)
    n = send_ref.shape[0]
    share = hidden_ref.shape[0] // n
    third = share // 3
    some = n // OUT_PIECES
    low = lax.broadcasted_iota(jnp.int32, (some, third, LANES), 2) < HALF
    copies = []
    for i in range(OUT_PIECES):
        here = slice(i * some, (i + 1) * some)
        total = jnp.dot(
            hidden_ref[i * some * share : (i + 1) * some * share],
            scaled,
            preferred_element_type=F32,
        ).reshape(some, share, 3 * LANES)
        send_ref[here, :share] = total[:, :, :LANES].astype(BF16)
        send_ref[here, share : 2 * share] = total[:, :, LANES : 2 * LANES].astype(BF16)
        last = total[:, :, 2 * LANES :]
        swapped = pltpu.roll(last[:, third : 2 * third], HALF, 2)
        mixed = jnp.where(low, last[:, :third], swapped)
        send_ref[here, 2 * share : 2 * share + third] = mixed.astype(BF16)
        send_ref[here, 2 * share + third :] = last[:, 2 * third :].astype(BF16)
        copies.append(pltpu.make_async_copy(send_ref.at[here], out_ref.at[here], left.at[i]))
        copies[-1].start()
    for copy in copies:
        copy.wait()


def sum_kernel(n_0, n_1, terms_ref, out_ref):
    share = out_ref.shape[0]
    third = share // 3
    n = 2 * n_0
    low = lax.broadcasted_iota(jnp.int32, (third, LANES), 1) < HALF

    def put(row, tile, value):
        out_ref[row : row + value.shape[0], tile * LANES : (tile + 1) * LANES] = value.astype(BF16)

    for k in range(n_0):
        ends = []
        for j in range(2):
            total = None
            for i in range(n_1):
                term = terms_ref[(k * n_1 + i) * 2 + j].astype(F32)
                total = term if total is None else total + term
            tile = 2 * (2 * k + j)
            put(0, tile, total[:share])
            put(0, tile + 1, total[share : 2 * share])
            ends.append((total[2 * share : 2 * share + third], total[2 * share + third :]))
        (mixed_0, last_0), (mixed_1, last_1) = ends
        tile = 2 * n + k
        put(0, tile, jnp.where(low, mixed_0, pltpu.roll(mixed_1, HALF, 1)))
        put(third, tile, jnp.where(low, pltpu.roll(mixed_0, HALF, 1), mixed_1))
        put(2 * third, tile, jnp.where(low, last_0, pltpu.roll(last_1, HALF, 1)))


def grads_kernel(*refs):
    sources, grad_gate_ref, grad_up_ref = refs[:4], refs[4], refs[5]
    (scaled_ref, gate_ref, up_ref, weight_ref), arrived = refs[6:10], refs[10]
    copies = [
        pltpu.make_async_copy(source, place, arrived.at[i])
        for i, (source, place) in enumerate(zip(sources[:3], refs[6:9]))
    ]
    units = weight_ref.shape[0]
    piece = units // PIECES
    for i in range(PIECES):
        rows = pl.ds(i * piece, piece)
        copies.append(
            pltpu.make_async_copy(sources[3].at[rows], weight_ref.at[rows], arrived.at[3 + i])
        )
    for copy in copies:
        copy.start()
    for copy in copies[:3]:
        copy.wait()
    for i in range(PIECES):
        copies[3 + i].wait()
        rows = slice(i * piece, (i + 1) * piece)
        d_hidden = lax.dot_general(
            scaled_ref[...],
            weight_ref[rows],
            (((1,), (1,)), ((), ())),
            preferred_element_type=F32,
        )
        gate, up = gate_ref[:, rows].astype(F32), up_ref[:, rows].astype(F32)
        sigmoid = jax.nn.sigmoid(gate)
        slope = sigmoid * (1.0 + gate * (1.0 - sigmoid))
        grad_gate_ref[:, rows] = (d_hidden * up * slope).astype(BF16)
        grad_up_ref[:, rows] = (d_hidden * (gate * sigmoid)).astype(BF16)


def return_kernel(offsets, chips, me_ref, grad_p_ref, presel_ref, expert_ref, slot_ref, out_ref):
    tokens = presel_ref.shape[1]
    row = lax.broadcasted_iota(jnp.int32, (grad_p_ref.shape[0], tokens), 0)
    node = jnp.full(row.shape, -1)
    offsets = [o % chips for o in offsets]
    for i, offset in enumerate(offsets):
        if offset in offsets[:i]:
            continue
        for flip in range(2):
            held = lax.rem(me_ref[0] // 2 + offset, chips) * 2 + (me_ref[0] % 2 ^ flip)
            node = jnp.where(row == flip * len(offsets) + i, held, node)
    expert, slot, presel = expert_ref[...], slot_ref[...], presel_ref[...]
    slots = columns_of_routes(expert, slot, slot + 1)
    slot_ids = lax.broadcasted_iota(jnp.int32, (LANES, tokens), 0)
    here = jnp.concatenate(
        [
            jnp.where(presel[c : c + 1] == node, 1.0, 0.0)
            for c in range(PRESEL)
        ],
        axis=1,
    )
    by_slot = lax.dot_general(
        grad_p_ref[...],
        here,
        (((0,), (0,)), ((), ())),
        preferred_element_type=F32,
        precision=lax.Precision.HIGHEST,
    )
    result = jnp.zeros(out_ref.shape, F32)
    for c in range(PRESEL):
        values = by_slot[:, c * tokens : (c + 1) * tokens]
        value = jnp.sum(jnp.where(slot_ids + 1 == slots[c], values, 0.0), axis=0, keepdims=True)
        result += jnp.where((expert == c * EXP_NODE) & (slot >= 0), value, 0.0)
    out_ref[...] = result


HBM = pl.BlockSpec(memory_space=pltpu.HBM)
VMEM = pl.BlockSpec(memory_space=pltpu.VMEM)
SMEM = pl.BlockSpec(memory_space=pltpu.SMEM)


def call(kernel, out_shape, in_specs, scratch=(), vmem_mib=12, out_space=VMEM, aliases=None):
    many = isinstance(out_shape, (tuple, list))
    return pl.pallas_call(
        kernel,
        out_shape=out_shape,
        in_specs=in_specs,
        out_specs=[out_space] * len(out_shape)
        if many and not isinstance(out_space, list)
        else out_space,
        scratch_shapes=scratch,
        input_output_aliases=aliases or {},
        compiler_params=pltpu.CompilerParams(vmem_limit_bytes=vmem_mib << 20),
    )


def exchange(value, axes):
    return lax.all_to_all(value, axes, split_axis=0, concat_axis=0, tiled=True)


def step_of(
    out_grad, gate_prob, presel_nodes, route_expert, route_slot, gate_pre, up_pre, down_weight
):
    _, features = out_grad.shape
    capacity, units = gate_pre.shape
    n_node, n_0, n_1, n_2 = (lax.axis_size(a) for a in NODE_DP)
    team = n_0 * n_2
    group = team * n_1
    share = units // group
    shape = jax.ShapeDtypeStruct
    presel, expert, slot = presel_nodes.T, route_expert.T, route_slot.T
    routed = (out_grad, gate_prob.T, presel, expert, slot)

    chunks = (n_node, features // LANES * SRC_CAP + SRC_CAP // 2, LANES)
    send = call(
        route_kernel,
        shape(chunks, BF16),
        [HBM] * 5,
        [pltpu.VMEM(a.shape, a.dtype) for a in routed]
        + [pltpu.VMEM(chunks, BF16)]
        + [pltpu.SemaphoreType.DMA((5,)), pltpu.SemaphoreType.DMA((OUT_PIECES,))],
        out_space=HBM,
        vmem_mib=60,
    )(*routed)
    recv = exchange(send, "node")

    weight = down_weight[0]
    gate_rows = gate_pre.astype(F32)
    hidden = (gate_rows * jax.nn.sigmoid(gate_rows) * up_pre.astype(F32)).astype(BF16)
    near = lax.ppermute(hidden, "dp_2", [(0, 1), (1, 0)])
    hidden_pair = jnp.stack([hidden, near])
    hiddens = [hidden_pair]
    for k in range(1, n_0):
        hiddens.append(lax.ppermute(hidden_pair, "dp_0", [(i, (i + k) % n_0) for i in range(n_0)]))
    team_hidden = call(
        collect_kernel,
        shape((units, team * capacity), BF16),
        [SMEM] + [VMEM] * n_0,
        [pltpu.VMEM((team * capacity, units), F32)],
    )(jnp.stack([lax.axis_index(a) for a in TEAM]), *hiddens)
    slot_out = jnp.dot(hidden, weight, preferred_element_type=F32)

    part = (team, features * capacity // (team * LANES), LANES)
    scaled, parts, grad_p = call(
        land_kernel,
        [
            pltpu.HBM((capacity, features), BF16),
            pltpu.HBM(part, BF16),
            pltpu.VMEM((1, LANES), F32),
        ],
        [VMEM] * 2,
        [
            pltpu.VMEM((capacity, features), BF16),
            pltpu.VMEM(part, BF16),
            pltpu.SemaphoreType.DMA((1 + team,)),
        ],
        out_space=[HBM, HBM, VMEM],
    )(recv, slot_out)
    parts = exchange(parts, TEAM)

    sources = (scaled, gate_pre, up_pre, weight)
    grad_gate, grad_up = call(
        grads_kernel,
        [shape((capacity, units), BF16)] * 2,
        [HBM] * 4,
        [pltpu.VMEM(a.shape, a.dtype) for a in sources]
        + [pltpu.SemaphoreType.DMA((3 + PIECES,))],
        vmem_mib=60,
    )(*sources)

    terms = (group, 2 * share + 2 * share // 3, LANES)
    partial = call(
        partial_kernel,
        pltpu.HBM(terms, BF16),
        [VMEM] * 2,
        [pltpu.VMEM(terms, BF16), pltpu.SemaphoreType.DMA((OUT_PIECES,))],
        out_space=HBM,
    )(team_hidden, parts)
    terms = exchange(partial, DP)
    grad_down = call(
        functools.partial(sum_kernel, n_0, n_1), shape((share, features), BF16), [VMEM]
    )(terms)[None]

    chips = n_node // 2
    offsets = [0]
    for step in (3, 1):
        rows = [grad_p]
        for sign in (1, -1):
            pairs = [
                (2 * ((i + sign * step) % chips) + core, 2 * i + core)
                for i in range(chips)
                for core in range(2)
            ]
            rows.append(lax.ppermute(grad_p, "node", pairs))
        grad_p = jnp.concatenate(rows)
        offsets = offsets + [o + step for o in offsets] + [o - step for o in offsets]
    other = lax.ppermute(grad_p, "node", [(i, i ^ 1) for i in range(n_node)])
    grad_p = jnp.concatenate([grad_p, other])
    grad_prob = call(
        functools.partial(return_kernel, offsets, chips),
        shape(route_expert.shape[::-1], F32),
        [SMEM] + [VMEM] * 4,
    )(lax.axis_index("node")[None], grad_p, presel, expert, slot).T
    return (grad_gate, grad_up, grad_down, grad_prob)


def solution(mesh):
    finer = Mesh(mesh.devices.reshape(mesh.shape["node"], 4, 4, 2), NODE_DP)
    in_specs = (P(NODE_DP, None),) * 7 + (P("node", None, None),)
    out_specs = (
        P(NODE_DP, None),
        P(NODE_DP, None),
        P("node", DP, None),
        P(NODE_DP, None),
    )
    return jax.shard_map(
        step_of, mesh=finer, in_specs=in_specs, out_specs=out_specs, check_vma=False
    )
```

```python
import functools

import jax
import jax.numpy as jnp
from jax import lax
from jax.experimental import pallas as pl
from jax.experimental.pallas import tpu as pltpu
from jax.sharding import Mesh
from jax.sharding import PartitionSpec as P

EXP_NODE = 10
PRESEL = 3
SRC_CAP = 16
LANES = 128
DP = ("dp_0", "dp_1", "dp_2")
NODE = ("chip", "core")
NODE_DP = (*NODE, *DP)
TO_NODE = ("core", "chip")
TO_DP = ("dp_1", "dp_2", "dp_0")
TEAM = ("dp_0", "dp_2")
HALF = LANES // 2
PIECES = 3
OUT_PIECES = 4
F32 = jnp.float32
BF16 = jnp.bfloat16


def columns_of_routes(expert, slot, value):
    rows = []
    for c in range(PRESEL):
        named = (expert == c * EXP_NODE) & (slot >= 0)
        rows.append(jnp.sum(jnp.where(named, value, 0), axis=0, keepdims=True))
    return rows


def route_kernel(*refs):
    sources, out_ref, held, (send_ref, arrived, left) = refs[:5], refs[5], refs[6:11], refs[11:14]
    copies = [
        pltpu.make_async_copy(source, place, arrived.at[i])
        for i, (source, place) in enumerate(zip(sources, held))
    ]
    for copy in reversed(copies):
        copy.start()
    for copy in reversed(copies[1:]):
        copy.wait()
    og_ref, prob_ref, presel_ref, expert_ref, slot_ref = held
    tokens, features = og_ref.shape
    n_node = send_ref.shape[0]
    expert, slot, presel = expert_ref[...], slot_ref[...], presel_ref[...]
    slots = columns_of_routes(expert, slot, slot + 1)
    probs = columns_of_routes(expert, slot, prob_ref[...].astype(F32))
    row = lax.broadcasted_iota(jnp.int32, (n_node, tokens), 0)
    node_ids = lax.rem(row, n_node // 2) * 2 + row // (n_node // 2)
    slot_to = jnp.zeros((n_node, tokens), F32)
    prob_to = jnp.zeros((n_node, tokens), F32)
    for c in range(PRESEL):
        here = presel[c : c + 1] == node_ids
        slot_to += jnp.where(here, slots[c].astype(F32), 0.0)
        prob_to += jnp.where(here, probs[c], 0.0)
    sent = slot_to > 0.0
    before = lax.broadcasted_iota(jnp.int32, (tokens, tokens), 0) < lax.broadcasted_iota(
        jnp.int32, (tokens, tokens), 1
    )
    rank = jnp.dot(
        jnp.where(sent, 1.0, 0.0).astype(BF16),
        jnp.where(before, 1.0, 0.0).astype(BF16),
        preferred_element_type=F32,
    )
    rank = jnp.where(sent, rank, -1.0)
    place = lax.broadcasted_iota(jnp.int32, (n_node, SRC_CAP, tokens), 1).astype(F32)
    picked = rank[:, None, :] == place
    rows = n_node * SRC_CAP
    slot_rows = jnp.sum(jnp.where(picked, slot_to[:, None, :], 0.0), axis=2, keepdims=True)
    prob_rows = jnp.sum(jnp.where(picked, prob_to[:, None, :], 0.0), axis=2, keepdims=True)
    half = SRC_CAP // 2
    lane = lax.broadcasted_iota(jnp.int32, (n_node, half, LANES), 2)
    info = jnp.zeros((n_node, half, LANES), F32)
    for i, column in enumerate(
        (slot_rows[:, :half], prob_rows[:, :half], slot_rows[:, half:], prob_rows[:, half:])
    ):
        info = jnp.where(lane == i, column, info)
    tiles = features // LANES
    send_ref[:, tiles * SRC_CAP :] = info.astype(BF16)
    pick = jnp.where(picked, 1.0, 0.0).reshape(rows, tokens).astype(BF16)
    copies[0].wait()
    leaving = []
    some = n_node // OUT_PIECES
    for i in range(OUT_PIECES):
        here = slice(i * some, (i + 1) * some)
        taken = jnp.dot(
            pick[i * some * SRC_CAP : (i + 1) * some * SRC_CAP],
            og_ref[...],
            preferred_element_type=F32,
        )
        for k in range(tiles):
            send_ref[here, k * SRC_CAP : (k + 1) * SRC_CAP] = (
                taken[:, k * LANES : (k + 1) * LANES].reshape(some, SRC_CAP, LANES).astype(BF16)
            )
        leaving.append(pltpu.make_async_copy(send_ref.at[here], out_ref.at[here], left.at[i]))
        leaving[-1].start()
    for copy in leaving:
        copy.wait()


def land_kernel(
    recv_ref, slot_out_ref, scaled_out_ref, out_ref, grad_p_ref, scaled_ref, parts_ref, left
):
    capacity, features = scaled_ref.shape
    n_node = recv_ref.shape[0]
    rows = n_node * SRC_CAP
    info = recv_ref[:, features // LANES * SRC_CAP :].astype(F32)
    slot, prob = (
        jnp.concatenate([info[:, :, i : i + 1], info[:, :, i + 2 : i + 3]], axis=1).reshape(rows, 1)
        for i in range(2)
    )
    lane = lax.broadcasted_iota(jnp.int32, (rows, LANES), 1).astype(F32)
    landing = jnp.where(slot == lane + 1.0, 1.0, 0.0).T[:capacity].astype(BF16)

    def landed(value):
        return jnp.dot(landing, value, preferred_element_type=F32)

    def pair(tile):
        return landed(
            jnp.concatenate(
                [
                    recv_ref[:, i * SRC_CAP : (i + 1) * SRC_CAP].reshape(rows, LANES)
                    for i in (tile, tile + 1)
                ],
                axis=1,
            )
        )

    p = landed(jnp.where(lane < LANES, prob, 0.0).astype(BF16))
    n = parts_ref.shape[0]
    half = capacity // 2
    low = lax.broadcasted_iota(jnp.int32, (half, LANES), 1) < HALF
    sums = jnp.zeros((capacity, LANES), F32)

    def settle(dy, tile):
        value = p * dy
        here = slice(tile * LANES, (tile + 1) * LANES)
        scaled_ref[:, here] = value.astype(BF16)
        return value, dy * slot_out_ref[:, here]

    for tile in range(2 * n, features // LANES, 2):
        both = pair(tile)
        for i in range(2):
            own, term = settle(both[:, i * LANES : (i + 1) * LANES], tile + i)
            sums += term
            k = 2 * (tile + i - 2 * n)
            swapped = pltpu.roll(own, HALF, 1)
            parts_ref[k, 2 * capacity :] = jnp.where(low, own[:half], swapped[half:]).astype(BF16)
            parts_ref[k + 1, 2 * capacity :] = jnp.where(low, swapped[:half], own[half:]).astype(
                BF16
            )
    copies = []
    for k in range(n):
        both = pair(2 * k)
        for j in range(2):
            own, term = settle(both[:, j * LANES : (j + 1) * LANES], 2 * k + j)
            sums += term
            parts_ref[k, j * capacity : (j + 1) * capacity] = own.astype(BF16)
        copies.append(pltpu.make_async_copy(parts_ref.at[k], out_ref.at[k], left.at[k]))
        copies[-1].start()
    copies.append(pltpu.make_async_copy(scaled_ref, scaled_out_ref, left.at[n]))
    copies[-1].start()
    grad_p = jnp.sum(sums, axis=1, keepdims=True)
    row = lax.broadcasted_iota(jnp.int32, (capacity, LANES), 0)
    column = lax.broadcasted_iota(jnp.int32, (capacity, LANES), 1)
    grad_p_ref[...] = jnp.sum(jnp.where(row == column, grad_p, 0.0), axis=0, keepdims=True)
    for copy in copies:
        copy.wait()


def collect_kernel(me_ref, *refs):
    *hidden_refs, out_ref, rows_ref = refs
    n_0 = len(hidden_refs)
    capacity = hidden_refs[0].shape[1]
    for k, hidden_ref in enumerate(hidden_refs):
        for j in range(2):
            block = lax.rem(me_ref[0] - k + n_0, n_0) * 2 + (me_ref[1] ^ j)
            start = pl.multiple_of(block * capacity, capacity)
            rows_ref[pl.ds(start, capacity)] = hidden_ref[j].astype(F32)
    out_ref[...] = rows_ref[...].T.astype(BF16)


def partial_kernel(hidden_ref, parts_ref, out_ref, send_ref, left):
    team, rows, _ = parts_ref.shape
    capacity = rows * 2 // 5
    blocks = []
    for block in range(team):
        packed = parts_ref[block, 2 * capacity :].astype(F32)
        halves = jnp.concatenate([packed, pltpu.roll(packed, HALF, 1)]).astype(BF16)
        blocks.append(
            jnp.concatenate(
                [parts_ref[block, :capacity], parts_ref[block, capacity : 2 * capacity], halves],
                axis=1,
            )
        )
    scaled = jnp.concatenate(blocks)
    some, n_0 = send_ref.shape[:2]
    share = hidden_ref.shape[0] // (some * n_0)
    third = share // 3
    low = lax.broadcasted_iota(jnp.int32, (some, third, LANES), 2) < HALF
    copies = []
    for i in range(n_0):
        total = jnp.dot(
            hidden_ref[i * some * share : (i + 1) * some * share],
            scaled,
            preferred_element_type=F32,
        ).reshape(some, share, 3 * LANES)
        send_ref[:, i, :share] = total[:, :, :LANES].astype(BF16)
        send_ref[:, i, share : 2 * share] = total[:, :, LANES : 2 * LANES].astype(BF16)
        last = total[:, :, 2 * LANES :]
        swapped = pltpu.roll(last[:, third : 2 * third], HALF, 2)
        mixed = jnp.where(low, last[:, :third], swapped)
        send_ref[:, i, 2 * share : 2 * share + third] = mixed.astype(BF16)
        send_ref[:, i, 2 * share + third :] = last[:, 2 * third :].astype(BF16)
        copies.append(pltpu.make_async_copy(send_ref.at[:, i], out_ref.at[:, i], left.at[i]))
        copies[-1].start()
    for copy in copies:
        copy.wait()


def sum_kernel(n_0, n_1, terms_ref, out_ref):
    share = out_ref.shape[0]
    third = share // 3
    n = 2 * n_0
    low = lax.broadcasted_iota(jnp.int32, (third, LANES), 1) < HALF

    def put(row, tile, value):
        out_ref[row : row + value.shape[0], tile * LANES : (tile + 1) * LANES] = value.astype(BF16)

    for k in range(n_0):
        ends = []
        for j in range(2):
            total = None
            for i in range(n_1):
                term = terms_ref[(i * 2 + j) * n_0 + k].astype(F32)
                total = term if total is None else total + term
            tile = 2 * (2 * k + j)
            put(0, tile, total[:share])
            put(0, tile + 1, total[share : 2 * share])
            ends.append((total[2 * share : 2 * share + third], total[2 * share + third :]))
        (mixed_0, last_0), (mixed_1, last_1) = ends
        tile = 2 * n + k
        put(0, tile, jnp.where(low, mixed_0, pltpu.roll(mixed_1, HALF, 1)))
        put(third, tile, jnp.where(low, pltpu.roll(mixed_0, HALF, 1), mixed_1))
        put(2 * third, tile, jnp.where(low, last_0, pltpu.roll(last_1, HALF, 1)))


def grads_kernel(*refs):
    sources, grad_gate_ref, grad_up_ref = refs[:4], refs[4], refs[5]
    (scaled_ref, gate_ref, up_ref, weight_ref), arrived = refs[6:10], refs[10]
    copies = [
        pltpu.make_async_copy(source, place, arrived.at[i])
        for i, (source, place) in enumerate(zip(sources[:3], refs[6:9]))
    ]
    units = weight_ref.shape[0]
    piece = units // PIECES
    for i in range(PIECES):
        rows = pl.ds(i * piece, piece)
        copies.append(
            pltpu.make_async_copy(sources[3].at[rows], weight_ref.at[rows], arrived.at[3 + i])
        )
    for copy in copies:
        copy.start()
    for copy in copies[:3]:
        copy.wait()
    for i in range(PIECES):
        copies[3 + i].wait()
        rows = slice(i * piece, (i + 1) * piece)
        d_hidden = lax.dot_general(
            scaled_ref[...],
            weight_ref[rows],
            (((1,), (1,)), ((), ())),
            preferred_element_type=F32,
        )
        gate, up = gate_ref[:, rows].astype(F32), up_ref[:, rows].astype(F32)
        sigmoid = jax.nn.sigmoid(gate)
        slope = sigmoid * (1.0 + gate * (1.0 - sigmoid))
        grad_gate_ref[:, rows] = (d_hidden * up * slope).astype(BF16)
        grad_up_ref[:, rows] = (d_hidden * (gate * sigmoid)).astype(BF16)


def return_kernel(offsets, chips, me_ref, grad_p_ref, presel_ref, expert_ref, slot_ref, out_ref):
    tokens = presel_ref.shape[1]
    row = lax.broadcasted_iota(jnp.int32, (grad_p_ref.shape[0], tokens), 0)
    node = jnp.full(row.shape, -1)
    offsets = [o % chips for o in offsets]
    for i, offset in enumerate(offsets):
        if offset in offsets[:i]:
            continue
        for flip in range(2):
            held = lax.rem(me_ref[0] // 2 + offset, chips) * 2 + (me_ref[0] % 2 ^ flip)
            node = jnp.where(row == flip * len(offsets) + i, held, node)
    expert, slot, presel = expert_ref[...], slot_ref[...], presel_ref[...]
    slots = columns_of_routes(expert, slot, slot + 1)
    slot_ids = lax.broadcasted_iota(jnp.int32, (LANES, tokens), 0)
    here = jnp.concatenate(
        [
            jnp.where(presel[c : c + 1] == node, 1.0, 0.0)
            for c in range(PRESEL)
        ],
        axis=1,
    )
    by_slot = lax.dot_general(
        grad_p_ref[...],
        here,
        (((0,), (0,)), ((), ())),
        preferred_element_type=F32,
        precision=lax.Precision.HIGHEST,
    )
    result = jnp.zeros(out_ref.shape, F32)
    for c in range(PRESEL):
        values = by_slot[:, c * tokens : (c + 1) * tokens]
        value = jnp.sum(jnp.where(slot_ids + 1 == slots[c], values, 0.0), axis=0, keepdims=True)
        result += jnp.where((expert == c * EXP_NODE) & (slot >= 0), value, 0.0)
    out_ref[...] = result


HBM = pl.BlockSpec(memory_space=pltpu.HBM)
VMEM = pl.BlockSpec(memory_space=pltpu.VMEM)
SMEM = pl.BlockSpec(memory_space=pltpu.SMEM)


def call(kernel, out_shape, in_specs, scratch=(), vmem_mib=12, out_space=VMEM, aliases=None):
    many = isinstance(out_shape, (tuple, list))
    return pl.pallas_call(
        kernel,
        out_shape=out_shape,
        in_specs=in_specs,
        out_specs=[out_space] * len(out_shape)
        if many and not isinstance(out_space, list)
        else out_space,
        scratch_shapes=scratch,
        input_output_aliases=aliases or {},
        compiler_params=pltpu.CompilerParams(vmem_limit_bytes=vmem_mib << 20),
    )


def exchange(value, axes):
    return lax.all_to_all(value, axes, split_axis=0, concat_axis=0, tiled=True)


def step_of(
    out_grad, gate_prob, presel_nodes, route_expert, route_slot, gate_pre, up_pre, down_weight
):
    _, features = out_grad.shape
    capacity, units = gate_pre.shape
    chips, cores, n_0, n_1, n_2 = (lax.axis_size(a) for a in NODE_DP)
    n_node = chips * cores
    team = n_0 * n_2
    group = team * n_1
    share = units // group
    shape = jax.ShapeDtypeStruct
    presel, expert, slot = presel_nodes.T, route_expert.T, route_slot.T
    routed = (out_grad, gate_prob.T, presel, expert, slot)

    chunks = (n_node, features // LANES * SRC_CAP + SRC_CAP // 2, LANES)
    send = call(
        route_kernel,
        shape(chunks, BF16),
        [HBM] * 5,
        [pltpu.VMEM(a.shape, a.dtype) for a in routed]
        + [pltpu.VMEM(chunks, BF16)]
        + [pltpu.SemaphoreType.DMA((5,)), pltpu.SemaphoreType.DMA((OUT_PIECES,))],
        out_space=HBM,
        vmem_mib=60,
    )(*routed)
    recv = exchange(send, TO_NODE)

    weight = down_weight[0]
    gate_rows = gate_pre.astype(F32)
    hidden = (gate_rows * jax.nn.sigmoid(gate_rows) * up_pre.astype(F32)).astype(BF16)
    near = lax.ppermute(hidden, "dp_2", [(0, 1), (1, 0)])
    hidden_pair = jnp.stack([hidden, near])
    hiddens = [hidden_pair]
    for k in range(1, n_0):
        hiddens.append(lax.ppermute(hidden_pair, "dp_0", [(i, (i + k) % n_0) for i in range(n_0)]))
    team_hidden = call(
        collect_kernel,
        shape((units, team * capacity), BF16),
        [SMEM] + [VMEM] * n_0,
        [pltpu.VMEM((team * capacity, units), F32)],
    )(jnp.stack([lax.axis_index(a) for a in TEAM]), *hiddens)
    slot_out = jnp.dot(hidden, weight, preferred_element_type=F32)

    part = (team, features * capacity // (team * LANES), LANES)
    scaled, parts, grad_p = call(
        land_kernel,
        [
            pltpu.HBM((capacity, features), BF16),
            pltpu.HBM(part, BF16),
            pltpu.VMEM((1, LANES), F32),
        ],
        [VMEM] * 2,
        [
            pltpu.VMEM((capacity, features), BF16),
            pltpu.VMEM(part, BF16),
            pltpu.SemaphoreType.DMA((1 + team,)),
        ],
        out_space=[HBM, HBM, VMEM],
    )(recv, slot_out)
    parts = exchange(parts, TEAM)

    sources = (scaled, gate_pre, up_pre, weight)
    grad_gate, grad_up = call(
        grads_kernel,
        [shape((capacity, units), BF16)] * 2,
        [HBM] * 4,
        [pltpu.VMEM(a.shape, a.dtype) for a in sources]
        + [pltpu.SemaphoreType.DMA((3 + PIECES,))],
        vmem_mib=60,
    )(*sources)

    terms = (n_1 * n_2, n_0, 2 * share + 2 * share // 3, LANES)
    partial = call(
        partial_kernel,
        pltpu.HBM(terms, BF16),
        [VMEM] * 2,
        [pltpu.VMEM(terms, BF16), pltpu.SemaphoreType.DMA((n_0,))],
        out_space=HBM,
    )(team_hidden, parts)
    terms = exchange(partial.reshape(group, *terms[2:]), TO_DP)
    grad_down = call(
        functools.partial(sum_kernel, n_0, n_1), shape((share, features), BF16), [VMEM]
    )(terms)[None]

    offsets = [0]
    for step in (3, 1):
        rows = [grad_p]
        for sign in (1, -1):
            pairs = [
                (2 * ((i + sign * step) % chips) + core, 2 * i + core)
                for i in range(chips)
                for core in range(2)
            ]
            rows.append(lax.ppermute(grad_p, NODE, pairs))
        grad_p = jnp.concatenate(rows)
        offsets = offsets + [o + step for o in offsets] + [o - step for o in offsets]
    other = lax.ppermute(grad_p, NODE, [(i, i ^ 1) for i in range(n_node)])
    grad_p = jnp.concatenate([grad_p, other])
    grad_prob = call(
        functools.partial(return_kernel, offsets, chips),
        shape(route_expert.shape[::-1], F32),
        [SMEM] + [VMEM] * 4,
    )(lax.axis_index(NODE)[None], grad_p, presel, expert, slot).T
    return (grad_gate, grad_up, grad_down, grad_prob)


def solution(mesh):
    finer = Mesh(mesh.devices.reshape(mesh.shape["node"] // 2, 2, 4, 4, 2), NODE_DP)
    in_specs = (P(NODE_DP, None),) * 7 + (P(NODE, None, None),)
    out_specs = (
        P(NODE_DP, None),
        P(NODE_DP, None),
        P(NODE, DP, None),
        P(NODE_DP, None),
    )
    return jax.shard_map(
        step_of, mesh=finer, in_specs=in_specs, out_specs=out_specs, check_vma=False
    )
```

```python
import functools

import jax
import jax.numpy as jnp
from jax import lax
from jax.experimental import pallas as pl
from jax.experimental.pallas import tpu as pltpu
from jax.sharding import Mesh
from jax.sharding import PartitionSpec as P

EXP_NODE = 10
PRESEL = 3
SRC_CAP = 16
LANES = 128
DP = ("dp_0", "dp_1", "dp_2")
NODE = ("chip", "core")
NODE_DP = (*NODE, *DP)
TO_NODE = ("core", "chip")
TO_DP = ("dp_1", "dp_2", "dp_0")
TEAM = ("dp_0", "dp_2")
HALF = LANES // 2
PIECES = 3
OUT_PIECES = 2
F32 = jnp.float32
BF16 = jnp.bfloat16


def columns_of_routes(expert, slot, value):
    rows = []
    for c in range(PRESEL):
        named = (expert == c * EXP_NODE) & (slot >= 0)
        rows.append(jnp.sum(jnp.where(named, value, 0), axis=0, keepdims=True))
    return rows


def route_kernel(*refs):
    sources, out_ref, held, (send_ref, arrived, left) = refs[:5], refs[5], refs[6:11], refs[11:14]
    copies = [
        pltpu.make_async_copy(source, place, arrived.at[i])
        for i, (source, place) in enumerate(zip(sources, held))
    ]
    for copy in reversed(copies):
        copy.start()
    for copy in reversed(copies[1:]):
        copy.wait()
    og_ref, prob_ref, presel_ref, expert_ref, slot_ref = held
    tokens, features = og_ref.shape
    n_node = send_ref.shape[0]
    expert, slot, presel = expert_ref[...], slot_ref[...], presel_ref[...]
    slots = columns_of_routes(expert, slot, slot + 1)
    probs = columns_of_routes(expert, slot, prob_ref[...].astype(F32))
    row = lax.broadcasted_iota(jnp.int32, (n_node, tokens), 0)
    node_ids = lax.rem(row, n_node // 2) * 2 + row // (n_node // 2)
    slot_to = jnp.zeros((n_node, tokens), F32)
    prob_to = jnp.zeros((n_node, tokens), F32)
    for c in range(PRESEL):
        here = presel[c : c + 1] == node_ids
        slot_to += jnp.where(here, slots[c].astype(F32), 0.0)
        prob_to += jnp.where(here, probs[c], 0.0)
    sent = slot_to > 0.0
    before = lax.broadcasted_iota(jnp.int32, (tokens, tokens), 0) < lax.broadcasted_iota(
        jnp.int32, (tokens, tokens), 1
    )
    rank = jnp.dot(
        jnp.where(sent, 1.0, 0.0).astype(BF16),
        jnp.where(before, 1.0, 0.0).astype(BF16),
        preferred_element_type=F32,
    )
    rank = jnp.where(sent, rank, -1.0)
    place = lax.broadcasted_iota(jnp.int32, (n_node, SRC_CAP, tokens), 1).astype(F32)
    picked = rank[:, None, :] == place
    rows = n_node * SRC_CAP
    slot_rows = jnp.sum(jnp.where(picked, slot_to[:, None, :], 0.0), axis=2, keepdims=True)
    prob_rows = jnp.sum(jnp.where(picked, prob_to[:, None, :], 0.0), axis=2, keepdims=True)
    half = SRC_CAP // 2
    lane = lax.broadcasted_iota(jnp.int32, (n_node, half, LANES), 2)
    info = jnp.zeros((n_node, half, LANES), F32)
    for i, column in enumerate(
        (slot_rows[:, :half], prob_rows[:, :half], slot_rows[:, half:], prob_rows[:, half:])
    ):
        info = jnp.where(lane == i, column, info)
    tiles = features // LANES
    send_ref[:, tiles * SRC_CAP :] = info.astype(BF16)
    pick = jnp.where(picked, 1.0, 0.0).reshape(rows, tokens).astype(BF16)
    copies[0].wait()
    leaving = []
    some = n_node // OUT_PIECES
    for i in range(OUT_PIECES):
        here = slice(i * some, (i + 1) * some)
        taken = jnp.dot(
            pick[i * some * SRC_CAP : (i + 1) * some * SRC_CAP],
            og_ref[...],
            preferred_element_type=F32,
        )
        for k in range(tiles):
            send_ref[here, k * SRC_CAP : (k + 1) * SRC_CAP] = (
                taken[:, k * LANES : (k + 1) * LANES].reshape(some, SRC_CAP, LANES).astype(BF16)
            )
        leaving.append(pltpu.make_async_copy(send_ref.at[here], out_ref.at[here], left.at[i]))
        leaving[-1].start()
    for copy in leaving:
        copy.wait()


def land_kernel(
    recv_ref, slot_out_ref, scaled_out_ref, out_ref, grad_p_ref, scaled_ref, parts_ref, left
):
    capacity, features = scaled_ref.shape
    n_node = recv_ref.shape[0]
    rows = n_node * SRC_CAP
    info = recv_ref[:, features // LANES * SRC_CAP :].astype(F32)
    slot, prob = (
        jnp.concatenate([info[:, :, i : i + 1], info[:, :, i + 2 : i + 3]], axis=1).reshape(rows, 1)
        for i in range(2)
    )
    lane = lax.broadcasted_iota(jnp.int32, (rows, LANES), 1).astype(F32)
    landing = jnp.where(slot == lane + 1.0, 1.0, 0.0).T[:capacity].astype(BF16)

    def landed(value):
        return jnp.dot(landing, value, preferred_element_type=F32)

    def pair(tile):
        return landed(
            jnp.concatenate(
                [
                    recv_ref[:, i * SRC_CAP : (i + 1) * SRC_CAP].reshape(rows, LANES)
                    for i in (tile, tile + 1)
                ],
                axis=1,
            )
        )

    p = landed(jnp.where(lane < LANES, prob, 0.0).astype(BF16))
    n = parts_ref.shape[0]
    half = capacity // 2
    low = lax.broadcasted_iota(jnp.int32, (half, LANES), 1) < HALF
    sums = jnp.zeros((capacity, LANES), F32)

    def settle(dy, tile):
        value = p * dy
        here = slice(tile * LANES, (tile + 1) * LANES)
        scaled_ref[:, here] = value.astype(BF16)
        return value, dy * slot_out_ref[:, here]

    for tile in range(2 * n, features // LANES, 2):
        both = pair(tile)
        for i in range(2):
            own, term = settle(both[:, i * LANES : (i + 1) * LANES], tile + i)
            sums += term
            k = 2 * (tile + i - 2 * n)
            swapped = pltpu.roll(own, HALF, 1)
            parts_ref[k, 2 * capacity :] = jnp.where(low, own[:half], swapped[half:]).astype(BF16)
            parts_ref[k + 1, 2 * capacity :] = jnp.where(low, swapped[:half], own[half:]).astype(
                BF16
            )
    copies = []
    for k in range(n):
        both = pair(2 * k)
        for j in range(2):
            own, term = settle(both[:, j * LANES : (j + 1) * LANES], 2 * k + j)
            sums += term
            parts_ref[k, j * capacity : (j + 1) * capacity] = own.astype(BF16)
        copies.append(pltpu.make_async_copy(parts_ref.at[k], out_ref.at[k % 2 * (n // 2) + k // 2], left.at[k]))
        copies[-1].start()
    copies.append(pltpu.make_async_copy(scaled_ref, scaled_out_ref, left.at[n]))
    copies[-1].start()
    grad_p = jnp.sum(sums, axis=1, keepdims=True)
    row = lax.broadcasted_iota(jnp.int32, (capacity, LANES), 0)
    column = lax.broadcasted_iota(jnp.int32, (capacity, LANES), 1)
    grad_p_ref[...] = jnp.sum(jnp.where(row == column, grad_p, 0.0), axis=0, keepdims=True)
    for copy in copies:
        copy.wait()


def collect_kernel(me_ref, *refs):
    *hidden_refs, out_ref, rows_ref = refs
    n_0 = len(hidden_refs)
    capacity = hidden_refs[0].shape[1]
    for k, hidden_ref in enumerate(hidden_refs):
        for j in range(2):
            block = lax.rem(me_ref[0] - k + n_0, n_0) * 2 + (me_ref[1] ^ j)
            start = pl.multiple_of(block * capacity, capacity)
            rows_ref[pl.ds(start, capacity)] = hidden_ref[j].astype(F32)
    out_ref[...] = rows_ref[...].T.astype(BF16)


def partial_kernel(hidden_ref, parts_ref, out_ref, send_ref, left):
    team, rows, _ = parts_ref.shape
    capacity = rows * 2 // 5
    blocks = []
    for block in [k % 2 * (team // 2) + k // 2 for k in range(team)]:
        packed = parts_ref[block, 2 * capacity :].astype(F32)
        halves = jnp.concatenate([packed, pltpu.roll(packed, HALF, 1)]).astype(BF16)
        blocks.append(
            jnp.concatenate(
                [parts_ref[block, :capacity], parts_ref[block, capacity : 2 * capacity], halves],
                axis=1,
            )
        )
    scaled = jnp.concatenate(blocks)
    some, n_0 = send_ref.shape[:2]
    share = hidden_ref.shape[0] // (some * n_0)
    third = share // 3
    low = lax.broadcasted_iota(jnp.int32, (some, third, LANES), 2) < HALF
    copies = []
    step = n_0 // 2
    for i in range(0, n_0, step):
        total = jnp.dot(
            hidden_ref[i * some * share : (i + step) * some * share],
            scaled,
            preferred_element_type=F32,
        ).reshape(step, some, share, 3 * LANES)
        for k in range(step):
            each = total[k]
            send_ref[:, i + k, :share] = each[:, :, :LANES].astype(BF16)
            send_ref[:, i + k, share : 2 * share] = each[:, :, LANES : 2 * LANES].astype(BF16)
            last = each[:, :, 2 * LANES :]
            swapped = pltpu.roll(last[:, third : 2 * third], HALF, 2)
            mixed = jnp.where(low, last[:, :third], swapped)
            send_ref[:, i + k, 2 * share : 2 * share + third] = mixed.astype(BF16)
            send_ref[:, i + k, 2 * share + third :] = last[:, 2 * third :].astype(BF16)
            copies.append(
                pltpu.make_async_copy(
                    send_ref.at[:, i + k], out_ref.at[:, i + k], left.at[i + k]
                )
            )
            copies[-1].start()
    for copy in copies:
        copy.wait()


def sum_kernel(n_0, n_1, terms_ref, out_ref):
    share = out_ref.shape[0]
    third = share // 3
    n = 2 * n_0
    low = lax.broadcasted_iota(jnp.int32, (third, LANES), 1) < HALF

    def put(row, tile, value):
        out_ref[row : row + value.shape[0], tile * LANES : (tile + 1) * LANES] = value.astype(BF16)

    for k in range(n_0):
        ends = []
        for j in range(2):
            total = None
            for i in range(n_1):
                term = terms_ref[(i * 2 + j) * n_0 + k].astype(F32)
                total = term if total is None else total + term
            tile = 2 * (2 * k + j)
            put(0, tile, total[:share])
            put(0, tile + 1, total[share : 2 * share])
            ends.append((total[2 * share : 2 * share + third], total[2 * share + third :]))
        (mixed_0, last_0), (mixed_1, last_1) = ends
        tile = 2 * n + k
        put(0, tile, jnp.where(low, mixed_0, pltpu.roll(mixed_1, HALF, 1)))
        put(third, tile, jnp.where(low, pltpu.roll(mixed_0, HALF, 1), mixed_1))
        put(2 * third, tile, jnp.where(low, last_0, pltpu.roll(last_1, HALF, 1)))


def grads_kernel(*refs):
    sources, grad_gate_ref, grad_up_ref = refs[:4], refs[4], refs[5]
    (scaled_ref, gate_ref, up_ref, weight_ref), arrived = refs[6:10], refs[10]
    copies = [
        pltpu.make_async_copy(source, place, arrived.at[i])
        for i, (source, place) in enumerate(zip(sources[:3], refs[6:9]))
    ]
    units = weight_ref.shape[0]
    piece = units // PIECES
    for i in range(PIECES):
        rows = pl.ds(i * piece, piece)
        copies.append(
            pltpu.make_async_copy(sources[3].at[rows], weight_ref.at[rows], arrived.at[3 + i])
        )
    for copy in copies:
        copy.start()
    for copy in copies[:3]:
        copy.wait()
    for i in range(PIECES):
        copies[3 + i].wait()
        rows = slice(i * piece, (i + 1) * piece)
        d_hidden = lax.dot_general(
            scaled_ref[...],
            weight_ref[rows],
            (((1,), (1,)), ((), ())),
            preferred_element_type=F32,
        )
        gate, up = gate_ref[:, rows].astype(F32), up_ref[:, rows].astype(F32)
        sigmoid = jax.nn.sigmoid(gate)
        slope = sigmoid * (1.0 + gate * (1.0 - sigmoid))
        grad_gate_ref[:, rows] = (d_hidden * up * slope).astype(BF16)
        grad_up_ref[:, rows] = (d_hidden * (gate * sigmoid)).astype(BF16)


def return_kernel(offsets, chips, me_ref, grad_p_ref, presel_ref, expert_ref, slot_ref, out_ref):
    tokens = presel_ref.shape[1]
    row = lax.broadcasted_iota(jnp.int32, (grad_p_ref.shape[0], tokens), 0)
    node = jnp.full(row.shape, -1)
    offsets = [o % chips for o in offsets]
    for i, offset in enumerate(offsets):
        if offset in offsets[:i]:
            continue
        for flip in range(2):
            held = lax.rem(me_ref[0] // 2 + offset, chips) * 2 + (me_ref[0] % 2 ^ flip)
            node = jnp.where(row == flip * len(offsets) + i, held, node)
    expert, slot, presel = expert_ref[...], slot_ref[...], presel_ref[...]
    slots = columns_of_routes(expert, slot, slot + 1)
    slot_ids = lax.broadcasted_iota(jnp.int32, (LANES, tokens), 0)
    here = jnp.concatenate(
        [
            jnp.where(presel[c : c + 1] == node, 1.0, 0.0)
            for c in range(PRESEL)
        ],
        axis=1,
    )
    by_slot = lax.dot_general(
        grad_p_ref[...],
        here,
        (((0,), (0,)), ((), ())),
        preferred_element_type=F32,
        precision=lax.Precision.HIGHEST,
    )
    result = jnp.zeros(out_ref.shape, F32)
    for c in range(PRESEL):
        values = by_slot[:, c * tokens : (c + 1) * tokens]
        value = jnp.sum(jnp.where(slot_ids + 1 == slots[c], values, 0.0), axis=0, keepdims=True)
        result += jnp.where((expert == c * EXP_NODE) & (slot >= 0), value, 0.0)
    out_ref[...] = result


HBM = pl.BlockSpec(memory_space=pltpu.HBM)
VMEM = pl.BlockSpec(memory_space=pltpu.VMEM)
SMEM = pl.BlockSpec(memory_space=pltpu.SMEM)


def call(kernel, out_shape, in_specs, scratch=(), vmem_mib=12, out_space=VMEM, aliases=None):
    many = isinstance(out_shape, (tuple, list))
    return pl.pallas_call(
        kernel,
        out_shape=out_shape,
        in_specs=in_specs,
        out_specs=[out_space] * len(out_shape)
        if many and not isinstance(out_space, list)
        else out_space,
        scratch_shapes=scratch,
        input_output_aliases=aliases or {},
        compiler_params=pltpu.CompilerParams(vmem_limit_bytes=vmem_mib << 20),
    )


def exchange(value, axes):
    return lax.all_to_all(value, axes, split_axis=0, concat_axis=0, tiled=True)


def step_of(
    out_grad, gate_prob, presel_nodes, route_expert, route_slot, gate_pre, up_pre, down_weight
):
    _, features = out_grad.shape
    capacity, units = gate_pre.shape
    chips, cores, n_0, n_1, n_2 = (lax.axis_size(a) for a in NODE_DP)
    n_node = chips * cores
    team = n_0 * n_2
    group = team * n_1
    share = units // group
    shape = jax.ShapeDtypeStruct
    presel, expert, slot = presel_nodes.T, route_expert.T, route_slot.T
    routed = (out_grad, gate_prob.T, presel, expert, slot)

    chunks = (n_node, features // LANES * SRC_CAP + SRC_CAP // 2, LANES)
    send = call(
        route_kernel,
        shape(chunks, BF16),
        [HBM] * 5,
        [pltpu.VMEM(a.shape, a.dtype) for a in routed]
        + [pltpu.VMEM(chunks, BF16)]
        + [pltpu.SemaphoreType.DMA((5,)), pltpu.SemaphoreType.DMA((OUT_PIECES,))],
        out_space=HBM,
        vmem_mib=60,
    )(*routed)
    recv = exchange(send, TO_NODE)

    weight = down_weight[0]
    gate_rows = gate_pre.astype(F32)
    hidden = (gate_rows * jax.nn.sigmoid(gate_rows) * up_pre.astype(F32)).astype(BF16)
    near = lax.ppermute(hidden, "dp_2", [(0, 1), (1, 0)])
    hidden_pair = jnp.stack([hidden, near])
    hiddens = [hidden_pair]
    for k in range(1, n_0):
        hiddens.append(lax.ppermute(hidden_pair, "dp_0", [(i, (i + k) % n_0) for i in range(n_0)]))
    team_hidden = call(
        collect_kernel,
        shape((units, team * capacity), BF16),
        [SMEM] + [VMEM] * n_0,
        [pltpu.VMEM((team * capacity, units), F32)],
    )(jnp.stack([lax.axis_index(a) for a in TEAM]), *hiddens)
    slot_out = jnp.dot(hidden, weight, preferred_element_type=F32)

    part = (team, features * capacity // (team * LANES), LANES)
    scaled, parts, grad_p = call(
        land_kernel,
        [
            pltpu.HBM((capacity, features), BF16),
            pltpu.HBM(part, BF16),
            pltpu.VMEM((1, LANES), F32),
        ],
        [VMEM] * 2,
        [
            pltpu.VMEM((capacity, features), BF16),
            pltpu.VMEM(part, BF16),
            pltpu.SemaphoreType.DMA((1 + team,)),
        ],
        out_space=[HBM, HBM, VMEM],
    )(recv, slot_out)
    parts = exchange(parts, TEAM[::-1])

    sources = (scaled, gate_pre, up_pre, weight)
    grad_gate, grad_up = call(
        grads_kernel,
        [shape((capacity, units), BF16)] * 2,
        [HBM] * 4,
        [pltpu.VMEM(a.shape, a.dtype) for a in sources]
        + [pltpu.SemaphoreType.DMA((3 + PIECES,))],
        vmem_mib=60,
    )(*sources)

    terms = (n_1 * n_2, n_0, 2 * share + 2 * share // 3, LANES)
    partial = call(
        partial_kernel,
        pltpu.HBM(terms, BF16),
        [VMEM] * 2,
        [pltpu.VMEM(terms, BF16), pltpu.SemaphoreType.DMA((n_0,))],
        out_space=HBM,
    )(team_hidden, parts)
    terms = exchange(partial.reshape(group, *terms[2:]), TO_DP)
    grad_down = call(
        functools.partial(sum_kernel, n_0, n_1), shape((share, features), BF16), [VMEM]
    )(terms)[None]

    offsets = [0]
    for step in (3, 1):
        rows = [grad_p]
        for sign in (1, -1):
            pairs = [
                (2 * ((i + sign * step) % chips) + core, 2 * i + core)
                for i in range(chips)
                for core in range(2)
            ]
            rows.append(lax.ppermute(grad_p, NODE, pairs))
        grad_p = jnp.concatenate(rows)
        offsets = offsets + [o + step for o in offsets] + [o - step for o in offsets]
    other = lax.ppermute(grad_p, NODE, [(i, i ^ 1) for i in range(n_node)])
    grad_p = jnp.concatenate([grad_p, other])
    grad_prob = call(
        functools.partial(return_kernel, offsets, chips),
        shape(route_expert.shape[::-1], F32),
        [SMEM] + [VMEM] * 4,
    )(lax.axis_index(NODE)[None], grad_p, presel, expert, slot).T
    return (grad_gate, grad_up, grad_down, grad_prob)


def solution(mesh):
    finer = Mesh(mesh.devices.reshape(mesh.shape["node"] // 2, 2, 4, 4, 2), NODE_DP)
    in_specs = (P(NODE_DP, None),) * 7 + (P(NODE, None, None),)
    out_specs = (
        P(NODE_DP, None),
        P(NODE_DP, None),
        P(NODE, DP, None),
        P(NODE_DP, None),
    )
    return jax.shard_map(
        step_of, mesh=finer, in_specs=in_specs, out_specs=out_specs, check_vma=False
    )
```
